64 devices in a mesh: dp: 4 (over x, y), tp: 16 (over z, core).
Axes of the slice: x: 2, y: 2, z: 8, core: 2. Of those that a mesh axis runs over, the one named last changes fastest.
The devices are a block of a 4x4x8 slice.
Arguments:
- x_in: bfloat16 [24, 128, 4096], P('dp', 'tp'), parts along dimension 0
- seg_pos: int32 [24, 128], P('dp'), parts along dimension 0
- conv_state: bfloat16 [2, 24, 3, 4096], P(None, 'dp', None, 'tp'), parts along dimension 1
- lru_state: float32 [2, 24, 4096], P(None, 'dp', 'tp'), parts along dimension 1
- k_cache: bfloat16 [24, 2048, 256], P('dp'), parts along dimension 0
- v_cache: bfloat16 [24, 2048, 256], P('dp'), parts along dimension 0
- slot_pos: int32 [24, 2048], P('dp'), parts along dimension 0
- norm_scale: bfloat16 [6, 4096], replicated
- w_x: bfloat16 [2, 4096, 4096], P(None, None, 'tp')
- b_x: bfloat16 [2, 4096], P(None, 'tp')
- w_y: bfloat16 [2, 4096, 4096], P(None, None, 'tp')
- b_y: bfloat16 [2, 4096], P(None, 'tp')
- conv_w: bfloat16 [2, 4, 4096], P(None, None, 'tp')
- conv_b: bfloat16 [2, 4096], P(None, 'tp')
- w_a: bfloat16 [2, 16, 256, 256], P(None, 'tp')
- b_a: bfloat16 [2, 4096], P(None, 'tp')
- w_i: bfloat16 [2, 16, 256, 256], P(None, 'tp')
- b_i: bfloat16 [2, 4096], P(None, 'tp')
- a_param: float32 [2, 4096], P(None, 'tp')
- w_out: bfloat16 [2, 4096, 4096], P(None, 'tp')
- b_out: bfloat16 [2, 4096], replicated
- w_q: bfloat16 [4096, 4096], P(None, 'tp')
- w_k: bfloat16 [4096, 256], replicated
- w_v: bfloat16 [4096, 256], replicated
- w_o: bfloat16 [4096, 4096], P('tp')
- b_o: bfloat16 [4096], replicated
- w_1: bfloat16 [3, 4096, 12288], P(None, None, 'tp')
- b_1: bfloat16 [3, 12288], P(None, 'tp')
- w_2: bfloat16 [3, 4096, 12288], P(None, None, 'tp')
- b_2: bfloat16 [3, 12288], P(None, 'tp')
- w_d: bfloat16 [3, 12288, 4096], P(None, 'tp')
- b_d: bfloat16 [3, 4096], replicated
Outputs:
- output 1: bfloat16 [24, 128, 4096], P('dp', 'tp'), parts along dimension 0
- output 2: bfloat16 [2, 24, 3, 4096], P(None, 'dp', None, 'tp'), parts along dimension 1
- output 3: float32 [2, 24, 4096], P(None, 'dp', 'tp'), parts along dimension 1
- output 4: bfloat16 [24, 2048, 256], P('dp'), parts along dimension 0
- output 5: bfloat16 [24, 2048, 256], P('dp'), parts along dimension 0
- output 6: int32 [24, 2048], P('dp'), parts along dimension 0
There are 4 independent parts. The reference program is written for one: setup_inputs(seed, part) draws one part's arguments, and reference() takes and returns one part's arrays. A program takes and returns all parts, laid end to end along the dimension named above; an argument that names none is the same for every part.
All inputs are finite; a program needn't handle non-finite values.
Results may differ from the reference program's by a relative error of at most 0.02.
Values are sent between devices in bfloat16 or wider.
A program may use at most 768 MiB of HBM per device.

```python
import jax
import jax.numpy as jnp
from jax import lax

BATCH = 6
TOKENS = 128
D = 4096
L = 4096
HEADS = 16
FF = 12288
WINDOW = 2048
HEAD_DIM = 256
ROPE_DIM = 128
CONV_WIDTH = 4
GATE_BLOCK = L // HEADS


def normal_draw(key_in, shape_in, scale_in):
    return jax.random.normal(key_in, shape_in, jnp.float32) * scale_in


def draw_positions(pos_key):
    key_reset, key_lap, key_offset = jax.random.split(pos_key, 3)
    reset_at = jnp.minimum(jax.random.randint(key_reset, (BATCH,), TOKENS // 2, 2 * TOKENS), TOKENS)
    lap_count = jax.random.randint(key_lap, (BATCH,), 0, 3)
    offset_in = jax.random.randint(key_offset, (BATCH,), 0, WINDOW - TOKENS + 1)
    start_pos = lap_count * WINDOW + TOKENS - reset_at + offset_in
    token_idx = jnp.arange(TOKENS)[None, :]
    seg_pos = jnp.where(token_idx < reset_at[:, None], start_pos[:, None] + token_idx, token_idx - reset_at[:, None])
    slot_idx = jnp.arange(WINDOW)[None, :]
    last_pos = start_pos[:, None] - 1 - jnp.mod(start_pos[:, None] - 1 - slot_idx, WINDOW)
    slot_pos = jnp.where(last_pos >= 0, last_pos, -1)
    return seg_pos.astype(jnp.int32), slot_pos.astype(jnp.int32)


def setup_inputs(seed: int = 0, part: int = 0) -> dict:
    base_key = jax.random.key(seed)
    root_keys = jax.random.split(base_key, 2)
    own_keys = jax.random.split(jax.random.fold_in(root_keys[0], part), 8)
    weight_keys = jax.random.split(root_keys[1], 32)
    seg_pos, slot_pos = draw_positions(own_keys[0])
    seq_mean = normal_draw(own_keys[6], (BATCH, 1, HEAD_DIM), 1.0)
    q_width = HEADS * HEAD_DIM
    return {
        'x_in': normal_draw(own_keys[1], (BATCH, TOKENS, D), 1.0).astype(jnp.bfloat16),
        'seg_pos': seg_pos,
        'conv_state': normal_draw(own_keys[2], (2, BATCH, CONV_WIDTH - 1, L), 2.0).astype(jnp.bfloat16),
        'lru_state': normal_draw(own_keys[3], (2, BATCH, L), 1.0),
        'k_cache': normal_draw(own_keys[4], (BATCH, WINDOW, HEAD_DIM), 2.0).astype(jnp.bfloat16),
        'v_cache': (normal_draw(own_keys[5], (BATCH, WINDOW, HEAD_DIM), 1.0) + seq_mean).astype(jnp.bfloat16),
        'slot_pos': slot_pos,
        'norm_scale': normal_draw(weight_keys[0], (6, D), 0.3).astype(jnp.bfloat16),
        'w_x': normal_draw(weight_keys[1], (2, D, L), D ** -0.5).astype(jnp.bfloat16),
        'b_x': normal_draw(weight_keys[2], (2, L), 0.5).astype(jnp.bfloat16),
        'w_y': normal_draw(weight_keys[3], (2, D, L), D ** -0.5).astype(jnp.bfloat16),
        'b_y': normal_draw(weight_keys[4], (2, L), 0.5).astype(jnp.bfloat16),
        'conv_w': normal_draw(weight_keys[5], (2, CONV_WIDTH, L), 0.5).astype(jnp.bfloat16),
        'conv_b': normal_draw(weight_keys[6], (2, L), 0.3).astype(jnp.bfloat16),
        'w_a': normal_draw(weight_keys[7], (2, HEADS, GATE_BLOCK, GATE_BLOCK), GATE_BLOCK ** -0.5).astype(jnp.bfloat16),
        'b_a': normal_draw(weight_keys[8], (2, L), 1.0).astype(jnp.bfloat16),
        'w_i': normal_draw(weight_keys[9], (2, HEADS, GATE_BLOCK, GATE_BLOCK), GATE_BLOCK ** -0.5).astype(jnp.bfloat16),
        'b_i': normal_draw(weight_keys[10], (2, L), 0.5).astype(jnp.bfloat16),
        'a_param': jnp.log(jnp.expm1(jax.random.uniform(weight_keys[11], (2, L), jnp.float32, 1e-4, 1e-3))),
        'w_out': normal_draw(weight_keys[12], (2, L, D), L ** -0.5).astype(jnp.bfloat16),
        'b_out': normal_draw(weight_keys[13], (2, D), 0.3).astype(jnp.bfloat16),
        'w_q': normal_draw(weight_keys[14], (D, q_width), D ** -0.5).astype(jnp.bfloat16),
        'w_k': normal_draw(weight_keys[15], (D, HEAD_DIM), D ** -0.5).astype(jnp.bfloat16),
        'w_v': normal_draw(weight_keys[16], (D, HEAD_DIM), D ** -0.5).astype(jnp.bfloat16),
        'w_o': normal_draw(weight_keys[17], (q_width, D), q_width ** -0.5).astype(jnp.bfloat16),
        'b_o': normal_draw(weight_keys[18], (D,), 0.3).astype(jnp.bfloat16),
        'w_1': normal_draw(weight_keys[19], (3, D, FF), D ** -0.5).astype(jnp.bfloat16),
        'b_1': normal_draw(weight_keys[20], (3, FF), 0.5).astype(jnp.bfloat16),
        'w_2': normal_draw(weight_keys[21], (3, D, FF), D ** -0.5).astype(jnp.bfloat16),
        'b_2': normal_draw(weight_keys[22], (3, FF), 0.5).astype(jnp.bfloat16),
        'w_d': normal_draw(weight_keys[23], (3, FF, D), FF ** -0.5).astype(jnp.bfloat16),
        'b_d': normal_draw(weight_keys[24], (3, D), 0.3).astype(jnp.bfloat16),
    }


def rms_norm(hidden, norm_gain):
    hidden_f32 = hidden.astype(jnp.float32)
    inv_rms = lax.rsqrt(jnp.mean(hidden_f32 * hidden_f32, axis=-1, keepdims=True) + 1e-6)
    return (hidden_f32 * inv_rms * (1.0 + norm_gain.astype(jnp.float32))).astype(jnp.bfloat16)


def dense_proj(act_in, weight):
    flat_acts = act_in.reshape(-1, act_in.shape[-1])
    product = jnp.dot(flat_acts, weight, preferred_element_type=jnp.float32)
    return product.reshape(act_in.shape[:-1] + (weight.shape[-1],))


def residual_add(hidden, update, bias_row):
    return (hidden.astype(jnp.float32) + update.astype(jnp.float32) + bias_row.astype(jnp.float32)).astype(jnp.bfloat16)


def apply_rope(proj_f32, pos_exp):
    half_dim = ROPE_DIM // 2
    timescale = 10000.0 ** (2.0 * jnp.arange(half_dim).astype(jnp.float32) / ROPE_DIM)
    angle_rad = pos_exp.astype(jnp.float32) / timescale
    sin_a = jnp.sin(angle_rad)
    cos_a = jnp.cos(angle_rad)
    first_half = proj_f32[..., :half_dim]
    second_half = proj_f32[..., half_dim:ROPE_DIM]
    return jnp.concatenate([first_half * cos_a - second_half * sin_a, second_half * cos_a + first_half * sin_a, proj_f32[..., ROPE_DIM:]], axis=-1).astype(jnp.bfloat16)


def recurrent_block(normed, seg_pos, conv_prev, state_prev, w_x, b_x, w_y, b_y, conv_w, conv_b, w_a, b_a, w_i, b_i, a_param, w_out):
    gate_y = jax.nn.gelu(dense_proj(normed, w_y) + b_y.astype(jnp.float32), approximate=True).astype(jnp.bfloat16)
    branch_x = (dense_proj(normed, w_x) + b_x.astype(jnp.float32)).astype(jnp.bfloat16)
    padded = jnp.concatenate([conv_prev, branch_x], axis=1).astype(jnp.float32)
    conv_f32 = conv_b.astype(jnp.float32) + sum(padded[:, tap_idx:tap_idx + TOKENS] * conv_w[tap_idx].astype(jnp.float32) for tap_idx in range(CONV_WIDTH))
    conv_bf = conv_f32.astype(jnp.bfloat16)
    blocks = conv_bf.astype(jnp.float32).reshape(BATCH, TOKENS, HEADS, GATE_BLOCK)
    gate_r = jax.nn.sigmoid(jnp.einsum('bchi,hij->bchj', blocks, w_a.astype(jnp.float32)).reshape(BATCH, TOKENS, L) + b_a.astype(jnp.float32))
    gate_i = jax.nn.sigmoid(jnp.einsum('bchi,hij->bchj', blocks, w_i.astype(jnp.float32)).reshape(BATCH, TOKENS, L) + b_i.astype(jnp.float32))
    decay_a = jnp.exp(-8.0 * gate_r * jax.nn.softplus(a_param))
    is_reset = (seg_pos == 0)[:, :, None]
    multiplier = jnp.where(is_reset, 1.0, jnp.sqrt(1.0 - decay_a * decay_a))
    decay_a = jnp.where(is_reset, 0.0, decay_a)
    drive_in = conv_bf.astype(jnp.float32) * gate_i * multiplier

    def lru_step(h_carry, step_in):
        new_h = step_in[0] * h_carry + step_in[1]
        return new_h, new_h

    last_h, hidden_seq = lax.scan(lru_step, state_prev, (jnp.swapaxes(decay_a, 0, 1), jnp.swapaxes(drive_in, 0, 1)))
    hidden_seq = jnp.swapaxes(hidden_seq, 0, 1)
    mixed_hy = (hidden_seq * gate_y.astype(jnp.float32)).astype(jnp.bfloat16)
    return dense_proj(mixed_hy, w_out), branch_x[:, TOKENS - (CONV_WIDTH - 1):], last_h


def attention_block(normed, seg_pos, k_cache, v_cache, slot_pos, w_q, w_k, w_v, w_o):
    query_rot = apply_rope(dense_proj(normed, w_q).reshape(BATCH, TOKENS, HEADS, HEAD_DIM), seg_pos[:, :, None, None])
    key_new = apply_rope(dense_proj(normed, w_k), seg_pos[:, :, None])
    value_new = dense_proj(normed, w_v).astype(jnp.bfloat16)

    def one_sequence(seq_in):
        q_seq, k_seq, v_seq, k_old, v_old, slot_seq, pos_seq = seq_in
        doc_id = jnp.cumsum((pos_seq == 0).astype(jnp.int32))
        diff_old = pos_seq[:, None] - slot_seq[None, :]
        mask_old = (slot_seq[None, :] >= 0) & (diff_old >= 0) & (diff_old < WINDOW) & (doc_id[:, None] == 0)
        diff_new = pos_seq[:, None] - pos_seq[None, :]
        mask_new = (diff_new >= 0) & (diff_new < WINDOW) & (doc_id[:, None] == doc_id[None, :])

        def one_head(q_head):
            score_old = jnp.where(mask_old, jnp.dot(q_head, k_old.T, preferred_element_type=jnp.float32) / 16.0, -1e30)
            score_new = jnp.where(mask_new, jnp.dot(q_head, k_seq.T, preferred_element_type=jnp.float32) / 16.0, -1e30)
            row_max = jnp.maximum(score_old.max(axis=-1), score_new.max(axis=-1))[:, None]
            exp_old = jnp.exp(score_old - row_max)
            exp_new = jnp.exp(score_new - row_max)
            denom_sum = exp_old.sum(axis=-1, keepdims=True) + exp_new.sum(axis=-1, keepdims=True)
            prob_old = (exp_old / denom_sum).astype(jnp.bfloat16)
            prob_new = (exp_new / denom_sum).astype(jnp.bfloat16)
            head_out = jnp.dot(prob_old, v_old, preferred_element_type=jnp.float32) + jnp.dot(prob_new, v_seq, preferred_element_type=jnp.float32)
            return head_out.astype(jnp.bfloat16)

        return lax.map(one_head, jnp.swapaxes(q_seq, 0, 1))

    attn_out = lax.map(one_sequence, (query_rot, key_new, value_new, k_cache, v_cache, slot_pos, seg_pos))
    attn_out = jnp.swapaxes(attn_out, 1, 2).reshape(BATCH, TOKENS, HEADS * HEAD_DIM)
    attn_proj = dense_proj(attn_out, w_o)
    batch_idx = jnp.arange(BATCH)[:, None]
    slot_new = jnp.mod(seg_pos, WINDOW)
    k_out = k_cache.at[batch_idx, slot_new].set(key_new)
    v_out = v_cache.at[batch_idx, slot_new].set(value_new)
    slot_out = slot_pos.at[batch_idx, slot_new].set(seg_pos)
    return attn_proj, k_out, v_out, slot_out


def mlp_block(normed, w_1, b_1, w_2, b_2, w_d):
    gate_val = jax.nn.gelu(dense_proj(normed, w_1) + b_1.astype(jnp.float32), approximate=True)
    up_val = dense_proj(normed, w_2) + b_2.astype(jnp.float32)
    return dense_proj((gate_val * up_val).astype(jnp.bfloat16), w_d)


def reference(x_in, seg_pos, conv_state, lru_state, k_cache, v_cache, slot_pos, norm_scale, w_x, b_x, w_y, b_y, conv_w, conv_b, w_a, b_a, w_i, b_i, a_param, w_out, b_out, w_q, w_k, w_v, w_o, b_o, w_1, b_1, w_2, b_2, w_d, b_d):
    hidden = x_in
    conv_list = []
    lru_list = []
    for layer_idx in range(2):
        rec_out, conv_new, lru_new = recurrent_block(rms_norm(hidden, norm_scale[2 * layer_idx]), seg_pos, conv_state[layer_idx], lru_state[layer_idx], w_x[layer_idx], b_x[layer_idx], w_y[layer_idx], b_y[layer_idx], conv_w[layer_idx], conv_b[layer_idx], w_a[layer_idx], b_a[layer_idx], w_i[layer_idx], b_i[layer_idx], a_param[layer_idx], w_out[layer_idx])
        hidden = residual_add(hidden, rec_out, b_out[layer_idx])
        mlp_out = mlp_block(rms_norm(hidden, norm_scale[2 * layer_idx + 1]), w_1[layer_idx], b_1[layer_idx], w_2[layer_idx], b_2[layer_idx], w_d[layer_idx])
        hidden = residual_add(hidden, mlp_out, b_d[layer_idx])
        conv_list.append(conv_new)
        lru_list.append(lru_new)
    attn_proj, k_out, v_out, slot_out = attention_block(rms_norm(hidden, norm_scale[4]), seg_pos, k_cache, v_cache, slot_pos, w_q, w_k, w_v, w_o)
    hidden = residual_add(hidden, attn_proj, b_o)
    mlp_out = mlp_block(rms_norm(hidden, norm_scale[5]), w_1[2], b_1[2], w_2[2], b_2[2], w_d[2])
    hidden = residual_add(hidden, mlp_out, b_d[2])
    return (hidden, jnp.stack(conv_list), jnp.stack(lru_list), k_out, v_out, slot_out)
```

```python
import functools

import jax
import jax.numpy as jnp
from jax import lax
from jax.experimental import pallas as pl
from jax.experimental.pallas import tpu as pltpu
from jax.sharding import PartitionSpec as P

WINDOW = 2048
HEAD_DIM = 256
ROPE_DIM = 128
CONV_WIDTH = 4
SCORE_SCALE = 0.0625
NEG_BIG = -1e30
F32 = jnp.float32
BF16 = jnp.bfloat16

SLOT_REL = (0, -1, 1, -2, 2, -3, 3, 4)
NC = 4
HALF = NC // 2
UP_ORDER = (0, 1, 2, 3)
DOWN_ORDER = (2, 3, 0, 1)


def slot_of(rel):
    if rel == 0:
        return 0
    if rel in (4, -4):
        return 7
    return -2 * rel - 1 if rel < 0 else 2 * rel


class Net:
    def __init__(self, tp, rows, dim, g, pown, dsend, drecv, zsend, zrecv, ag_z, ag_d, rs_z, rs_d, send_z, send_d):
        self.me = lax.axis_index('tp')
        self.core = lax.rem(self.me, 2)
        self.chips = tp // 2
        self.chip = lax.div(self.me, 2)
        self.up = lax.rem(self.me + 2, tp)
        self.down = lax.rem(self.me + tp - 2, tp)
        self.partner = self.me + 1 - 2 * self.core
        self.rows = rows
        self.dim = dim
        self.cw = dim // NC
        self.g, self.pown, self.dsend, self.drecv, self.zsend, self.zrecv = g, pown, dsend, drecv, zsend, zrecv
        self.ag_z, self.ag_d, self.rs_z, self.rs_d, self.send_z, self.send_d = ag_z, ag_d, rs_z, rs_d, send_z, send_d

    def barrier(self):
        sem = pltpu.get_barrier_semaphore()
        for other in (self.up, self.down, self.partner):
            pl.semaphore_signal(sem, inc=1, device_id={'tp': other}, device_id_type=pl.DeviceIdType.MESH)
        pl.semaphore_wait(sem, 3)

    def cols(self, ch):
        return pl.ds(ch * self.cw, self.cw)

    def remote(self, src, dst, send, recv, dev):
        return pltpu.make_async_remote_copy(src_ref=src, dst_ref=dst, send_sem=send, recv_sem=recv, device_id={'tp': dev}, device_id_type=pl.DeviceIdType.MESH)

    def ag_hop(self, way, d, ch):
        sign = -1 if way == 0 else 1
        src, dst = slot_of(sign * (d - 1)), slot_of(sign * d)
        return self.remote(self.g.at[2 * src + self.core, :, self.cols(ch)], self.g.at[2 * dst + self.core, :, self.cols(ch)],
                           self.send_z.at[way, d - 1, ch], self.ag_z.at[way, d - 1, ch], self.up if way == 0 else self.down)

    def ag_pair(self, slot, ch):
        ref = self.g.at[2 * slot + self.core, :, self.cols(ch)]
        return self.remote(ref, ref, self.send_d.at[slot, ch], self.ag_d.at[slot, ch], self.partner)

    def rs_pair(self, slot, ch):
        return self.remote(self.dsend.at[slot, :, self.cols(ch)], self.drecv.at[slot, :, self.cols(ch)],
                           self.send_d.at[slot, ch], self.rs_d.at[slot, ch], self.partner)

    def rs_hop(self, way, d, ch):
        return self.remote(self.zsend.at[way, d - 1, :, self.cols(ch)], self.zrecv.at[way, d - 1, :, self.cols(ch)],
                           self.send_z.at[way, d - 1, ch], self.rs_z.at[way, d - 1, ch], self.up if way == 0 else self.down)

    def last_hop(self, way, ch):
        return ch < HALF if way == 0 else ch >= HALF

    def hops(self):
        for way in range(2):
            for d in range(1, 5):
                for ch in range(NC):
                    if d < 4 or self.last_hop(way, ch):
                        yield way, d, ch

    def abs_chip(self, rel):
        return lax.rem(self.chip + (rel + self.chips), self.chips)

    def wait_pair(self, slots):
        for slot in slots:
            for ch in range(NC):
                self.ag_pair(slot, ch).wait_recv()

    def gather(self, run_pass):
        for p in range(NC):
            self.ag_hop(0, 1, UP_ORDER[p]).start()
            self.ag_hop(1, 1, DOWN_ORDER[p]).start()
        for ch in range(NC):
            self.ag_pair(0, ch).start()
        self.wait_pair((0,))
        run_pass(0, 1)
        for d in range(1, 5):
            for p in range(NC if d < 4 else HALF):
                for way, order in ((0, UP_ORDER), (1, DOWN_ORDER)):
                    ch = order[p]
                    self.ag_hop(way, d, ch).wait_recv()
                    if d < 3 or (d == 3 and self.last_hop(way, ch)):
                        self.ag_hop(way, d + 1, ch).start()
                    self.ag_pair(slot_of(-d if way == 0 else d), ch).start()
                if p == 0 and d > 1:
                    self.wait_pair((2 * d - 3, 2 * d - 2))
                    run_pass(2 * d - 3, 2 * d - 1)
        self.wait_pair((7,))
        run_pass(7, 8)
        for way, d, ch in self.hops():
            self.ag_hop(way, d, ch).wait_send()
        for slot in range(8):
            for ch in range(NC):
                self.ag_pair(slot, ch).wait_send()

    def reduce(self, lhs_of, w_ref, finish):
        rows = self.rows
        sub = min(512, self.cw)

        def slots_of(d):
            return {4: (7,), 0: (0,)}.get(d, (slot_of(-d), slot_of(d)))

        def compute(d, ch):
            slots = slots_of(d)
            lhs = jnp.concatenate([lhs_of(s, self.core) for s in slots] + [lhs_of(s, 1 - self.core) for s in slots], axis=0)
            for t in range(self.cw // sub):
                span = pl.ds(ch * self.cw + t * sub, sub)
                out = jnp.dot(lhs, w_ref[:, span], preferred_element_type=F32)
                for i, s in enumerate(slots):
                    self.pown[s, :, span] = out[i * rows:(i + 1) * rows]
                    self.dsend[s, :, span] = out[(len(slots) + i) * rows:(len(slots) + i + 1) * rows].astype(BF16)
            for s in slots:
                self.rs_pair(s, ch).start()

        def combine(way, d, ch):
            s = slot_of(d if way == 0 else -d)
            self.rs_pair(s, ch).wait_recv()
            total = self.pown[s, :, self.cols(ch)] + self.drecv[s, :, self.cols(ch)].astype(F32)
            if d < 3 or (d == 3 and self.last_hop(way, ch)):
                self.rs_hop(way, d + 1, ch).wait_recv()
                total = total + self.zrecv[way, d, :, self.cols(ch)].astype(F32)
            self.zsend[way, d - 1, :, self.cols(ch)] = total.astype(BF16)
            self.rs_hop(way, d, ch).start()

        order = tuple(x for i in range(HALF) for x in (i, i + HALF))
        for ch in order:
            compute(4, ch)
        for ch in order[:HALF]:
            compute(3, ch)
        for p in range(HALF):
            combine(0, 4, p)
            combine(1, 4, HALF + p)
        for ch in order[HALF:]:
            compute(3, ch)
        for d in (3, 2, 1):
            for p in range(NC):
                combine(0, d, (p + HALF) % NC)
                combine(1, d, p)
                compute(d - 1, order[p])
        for ch in range(NC):
            self.rs_pair(0, ch).wait_recv()
            self.rs_hop(0, 1, ch).wait_recv()
            self.rs_hop(1, 1, ch).wait_recv()
            total = self.pown[0, :, self.cols(ch)] + self.drecv[0, :, self.cols(ch)].astype(F32)
            total = total + self.zrecv[0, 0, :, self.cols(ch)].astype(F32) + self.zrecv[1, 0, :, self.cols(ch)].astype(F32)
            finish(self.cols(ch), total)
        for way, d, ch in self.hops():
            self.rs_hop(way, d, ch).wait_send()
        for slot in range(8):
            for ch in range(NC):
                self.rs_pair(slot, ch).wait_send()


def comm_kernel(cfg, names, outs, scratch, *refs):
    r = dict(zip(names + outs + scratch, refs))
    x_ref = r['x']
    rows, dim = x_ref.shape
    net = Net(cfg['tp'], rows, dim, r['g'], r.get('pown'), r.get('dsend'), r.get('drecv'), r.get('zsend'), r.get('zrecv'),
              r['ag_z'], r['ag_d'], r['rs_z'], r['rs_d'], r['send_z'], r['send_d'])
    loads = {}
    for i, (key, src, layer) in enumerate(cfg['loads']):
        view = r[src] if layer is None else r[src].at[layer]
        loads[key] = pltpu.make_async_copy(view, r[key], r['w_sem'].at[i])
        loads[key].start()
    net.barrier()
    xbuf = r['xbuf']
    xbuf[...] = x_ref[...]
    eps = 1e-6

    def normalize(idx):
        gain = 1.0 + r['norm'][idx:idx + 1, :].astype(F32)

        def body(i, carry):
            span = pl.ds(pl.multiple_of(i * 16, 16), 16)
            h = xbuf[span, :].astype(F32)
            inv = lax.rsqrt(jnp.mean(h * h, axis=-1, keepdims=True) + eps)
            r['g'][net.core, span, :] = (h * inv * gain).astype(BF16)
            return carry
        lax.fori_loop(0, rows // 16, body, 0)

    def finish_with(bias_ref, idx):
        def finish(cols, total):
            bias = bias_ref[idx:idx + 1, cols].astype(F32)
            xbuf[:, cols] = (xbuf[:, cols].astype(F32) + total + bias).astype(BF16)
        return finish

    def block_of(first, last):
        return r['g'][2 * first:2 * last].reshape((last - first) * 2 * rows, dim)

    if cfg['pre'] is not None:
        r['apre'][...] = r['mid'][...].astype(BF16)
        loads['w_pre'].wait()

        def lhs_pre(slot, core):
            blk = 2 * net.abs_chip(SLOT_REL[slot]) + core
            return r['apre'][pl.ds(pl.multiple_of(blk * rows, 16), rows), :]
        net.reduce(lhs_pre, r['w_pre'], finish_with(r['b_pre'], cfg['pre']))

    if cfg['mlp'] is not None:
        m = cfg['mlp']
        normalize(2 * m + 1)
        pending = ['w_1s', 'w_2s']

        def mlp_pass(first, last):
            while pending:
                loads[pending.pop()].wait()
            count = 2 * (last - first)
            ff = r['w_1s'].shape[1]

            def body(t, carry):
                cols = pl.ds(pl.multiple_of(t * 256, 256), 256)
                lhs = block_of(first, last)
                h1 = jnp.dot(lhs, r['w_1s'][:, cols], preferred_element_type=F32) + r['b_1'][m:m + 1, cols].astype(F32)
                h2 = jnp.dot(lhs, r['w_2s'][:, cols], preferred_element_type=F32) + r['b_2'][m:m + 1, cols].astype(F32)
                act = (jax.nn.gelu(h1, approximate=True) * h2).astype(BF16)
                r['act'][2 * first:2 * last, :, cols] = act.reshape(count, rows, 256)
                return carry
            lax.fori_loop(0, ff // 256, body, 0)
        net.gather(mlp_pass)
        loads['w_ds'].wait()
        net.reduce(lambda slot, core: r['act'][2 * slot + core], r['w_ds'], finish_with(r['b_d'], m))

    if cfg['post'] is not None:
        kind, idx = cfg['post']
        normalize(4 if kind == 'attn' else 2 * idx)
        waiting = [key for key, _, _ in cfg['loads'] if key.startswith('p_')]

        def post_pass(first, last):
            while waiting:
                loads[waiting.pop()].wait()
            lhs = block_of(first, last)
            spans = [pl.ds(pl.multiple_of(net.abs_chip(SLOT_REL[s]) * 2 * rows, 16), 2 * rows) for s in range(first, last)]

            def put(ref, value, rope=False):
                for i, span in enumerate(spans):
                    v = value[i * 2 * rows:(i + 1) * 2 * rows]
                    if rope:
                        lo = v[:, :ROPE_DIM]
                        lo = lo * r['cos'][span, :] + pltpu.roll(lo, ROPE_DIM // 2, 1) * r['sin'][span, :]
                        v = jnp.concatenate([lo, v[:, ROPE_DIM:]], axis=1)
                    ref[span, :] = v.astype(BF16).astype(F32)
            if kind == 'rec':
                put(r['o_u'], jnp.dot(lhs, r['p_x'][...], preferred_element_type=F32) + r['b_x'][idx:idx + 1, :].astype(F32))
                put(r['o_y'], jax.nn.gelu(jnp.dot(lhs, r['p_y'][...], preferred_element_type=F32) + r['b_y'][idx:idx + 1, :].astype(F32), approximate=True))
            else:
                put(r['o_q'], jnp.dot(lhs, r['p_q'][...], preferred_element_type=F32), True)
                put(r['o_k'], jnp.dot(lhs, r['p_k'][...], preferred_element_type=F32), True)
                put(r['o_v'], jnp.dot(lhs, r['p_v'][...], preferred_element_type=F32))
        net.gather(post_pass)
    if 'o_x' in r:
        r['o_x'][...] = xbuf[...]


def comm_call(tp, ident, x, pre=None, mlp=None, post=None):
    rows, dim = x.shape
    vmem, hbm = pl.BlockSpec(memory_space=pltpu.VMEM), pl.BlockSpec(memory_space=pl.ANY)
    args, specs, names, loads, scratch = [], [], [], [], {}

    def add(name, value, spec):
        names.append(name)
        args.append(value)
        specs.append(spec)
    add('x', x, vmem)
    outs = {}
    flops = 0
    if pre is not None or mlp is not None:
        outs['o_x'] = jax.ShapeDtypeStruct((rows, dim), BF16)
        scratch['pown'] = pltpu.VMEM((8, rows, dim), F32)
        scratch['dsend'] = pltpu.VMEM((8, rows, dim), BF16)
        scratch['drecv'] = pltpu.VMEM((8, rows, dim), BF16)
        scratch['zsend'] = pltpu.VMEM((2, 4, rows, dim), BF16)
        scratch['zrecv'] = pltpu.VMEM((2, 4, rows, dim), BF16)
    if pre is not None:
        mid, b_idx, w_pre, layer, b_pre = pre
        add('mid', mid, vmem)
        add('h_pre', w_pre, hbm)
        add('b_pre', b_pre, vmem)
        loads.append(('w_pre', 'h_pre', layer))
        scratch['w_pre'] = pltpu.VMEM(w_pre.shape[-2:], BF16)
        scratch['apre'] = pltpu.VMEM(mid.shape, BF16)
        flops += 2 * mid.shape[0] * w_pre.shape[-2] * dim
    if mlp is not None:
        m, norm, w_1, b_1, w_2, b_2, w_d, b_d = mlp
        ff = w_1.shape[-1]
        for key, value in (('h_1', w_1), ('h_2', w_2), ('h_d', w_d)):
            add(key, value, hbm)
        for key, value in (('b_1', b_1), ('b_2', b_2), ('b_d', b_d)):
            add(key, value, vmem)
        loads += [('w_1s', 'h_1', m), ('w_2s', 'h_2', m), ('w_ds', 'h_d', m)]
        scratch['w_1s'] = pltpu.VMEM((dim, ff), BF16)
        scratch['w_2s'] = pltpu.VMEM((dim, ff), BF16)
        scratch['w_ds'] = pltpu.VMEM((ff, dim), BF16)
        scratch['act'] = pltpu.VMEM((tp, rows, ff), BF16)
        flops += 6 * tp * rows * ff * dim
    else:
        norm = post[2]
    add('norm', norm, vmem)
    if post is not None:
        kind, idx, _, weights, extras = post
        width = weights[0][1].shape[-1]
        for key, value, layer in weights:
            add('h_' + key, value, hbm)
            loads.append((key, 'h_' + key, layer))
            scratch[key] = pltpu.VMEM(value.shape[-2:], BF16)
            outs['o_' + key[2:] if kind == 'attn' else {'p_x': 'o_u', 'p_y': 'o_y'}[key]] = jax.ShapeDtypeStruct((tp * rows, width), F32)
            flops += 2 * tp * rows * dim * width
        for key, value in extras:
            add(key, value, vmem)
    scratch['g'] = pltpu.VMEM((tp, rows, dim), BF16)
    scratch['xbuf'] = pltpu.VMEM((rows, dim), BF16)
    for key in ('ag_z', 'rs_z', 'send_z'):
        scratch[key] = pltpu.SemaphoreType.DMA((2, 4, NC))
    for key in ('ag_d', 'rs_d', 'send_d'):
        scratch[key] = pltpu.SemaphoreType.DMA((8, NC))
    scratch['w_sem'] = pltpu.SemaphoreType.DMA((len(loads),))
    cfg = dict(tp=tp, loads=tuple(loads), pre=None if pre is None else pre[1], mlp=None if mlp is None else mlp[0],
               post=None if post is None else (post[0], post[1]))
    result = pl.pallas_call(
        functools.partial(comm_kernel, cfg, names, list(outs), list(scratch)),
        out_shape=tuple(outs.values()),
        in_specs=specs,
        out_specs=tuple(vmem for _ in outs),
        scratch_shapes=list(scratch.values()),
        compiler_params=pltpu.CompilerParams(collective_id=ident, has_side_effects=True, vmem_limit_bytes=66 * 1000 * 1000),
        cost_estimate=pl.CostEstimate(flops=flops, bytes_accessed=flops // 1500, transcendentals=0),
        name='ring_' + str(ident),
    )(*args)
    return dict(zip(outs, result))


def rec_kernel(layer, seqs, u_ref, y_ref, pos_ref, cs_ref, ls_ref, cw_ref, cb_ref, wa_ref, ba_ref, wi_ref, bi_ref, sp_ref, hy_ref, co_ref, lo_ref, pad):
    blocks = u_ref.shape[0]
    toks = blocks * 8
    width = u_ref.shape[-1]

    def one_seq(s, carry):
        u = u_ref[:, s].reshape(toks, width)
        pad[8:8 + toks, :] = u
        pad[5:8, :] = cs_ref[s].astype(F32)
        co_ref[s] = u[toks - 3:, :].astype(BF16)
        total = jnp.zeros((toks, width), F32)
        for j in range(CONV_WIDTH):
            total = total + pad[5 + j:5 + j + toks, :] * cw_ref[layer, j:j + 1, :].astype(F32)
        conv = (total + cb_ref[layer:layer + 1, :].astype(F32)).astype(BF16)
        gate_r = jax.nn.sigmoid(jnp.dot(conv, wa_ref[0], preferred_element_type=F32) + ba_ref[layer:layer + 1, :].astype(F32))
        gate_i = jax.nn.sigmoid(jnp.dot(conv, wi_ref[0], preferred_element_type=F32) + bi_ref[layer:layer + 1, :].astype(F32))
        decay = jnp.exp(-8.0 * gate_r * sp_ref[layer:layer + 1, :])
        reset = pos_ref[s] == 0
        mult = jnp.where(reset, 1.0, jnp.sqrt(1.0 - decay * decay))
        decay = jnp.where(reset, 0.0, decay)
        drive = conv.astype(F32) * gate_i * mult
        a = decay.reshape(blocks, 8, width)
        b = drive.reshape(blocks, 8, width)
        row = lax.broadcasted_iota(jnp.int32, (blocks, 8, width), 1)
        for k in (1, 2, 4):
            inside = row >= k
            a_sh = jnp.where(inside, pltpu.roll(a, k, 1), 1.0)
            b_sh = jnp.where(inside, pltpu.roll(b, k, 1), 0.0)
            b = a * b_sh + b
            a = a * a_sh
        state = ls_ref[pl.ds(s, 1), :]
        for blk in range(blocks):
            h = a[blk] * state + b[blk]
            state = h[7:8, :]
            hy_ref[blk, s] = (h * y_ref[blk, s]).astype(BF16).astype(F32)
        lo_ref[pl.ds(s, 1), :] = state
        return carry
    lax.fori_loop(0, seqs, one_seq, 0)


def rec_call(layer, u, y, pos_col, conv_state, lru_state, conv_w, conv_b, w_a, b_a, w_i, b_i, soft):
    seqs = pos_col.shape[0]
    toks = pos_col.shape[1]
    width = u.shape[-1]
    blocks = toks // 8
    shape4 = (blocks, seqs, 8, width)
    full = pl.BlockSpec(memory_space=pltpu.VMEM)
    layer_spec = lambda a: pl.BlockSpec((None,) + a.shape[1:], functools.partial(lambda n, i: (layer,) + (0,) * n, a.ndim - 1))
    whole = lambda a: pl.BlockSpec(a.shape, functools.partial(lambda n, i: (0,) * n, a.ndim))
    out_shape = (jax.ShapeDtypeStruct(shape4, F32), jax.ShapeDtypeStruct((seqs, 3, width), BF16), jax.ShapeDtypeStruct((seqs, width), F32))
    args = (u.reshape(shape4), y.reshape(shape4), pos_col, conv_state, lru_state, conv_w, conv_b, w_a, b_a, w_i, b_i, soft)
    per_layer = {3, 4, 7, 9}
    return pl.pallas_call(
        functools.partial(rec_kernel, layer, seqs),
        grid=(1,),
        out_shape=out_shape,
        in_specs=[layer_spec(a) if i in per_layer else whole(a) for i, a in enumerate(args)],
        out_specs=tuple(whole(a) for a in out_shape),
        scratch_shapes=[pltpu.VMEM((toks + 8, width), F32)],
        cost_estimate=pl.CostEstimate(flops=4 * toks * seqs * width * width, bytes_accessed=16 * toks * seqs * width, transcendentals=0),
        name='recurrence_' + str(layer),
    )(*args)


def attn_kernel(q_ref, k_ref, v_ref, kc_ref, vc_ref, slot_ref, pos_row_ref, pos_col_ref, doc_row_ref, doc_col_ref, o_ref, ko_ref, vo_ref, so_ref):
    blocks, _, _, width = q_ref.shape
    toks = blocks * 8
    q = q_ref[...].reshape(toks, width).astype(BF16)
    kn = k_ref[...].reshape(toks, width).astype(BF16)
    vn = v_ref[...].reshape(toks, width).astype(BF16)
    kc, vc = kc_ref[0], vc_ref[0]
    slot = slot_ref[0]
    pos_row, pos_col, doc_row, doc_col = pos_row_ref[0], pos_col_ref[0], doc_row_ref[0], doc_col_ref[0]
    contract = (((1,), (1,)), ((), ()))
    diff_old = pos_col - slot
    keep_old = (slot >= 0) & (diff_old >= 0) & (diff_old < WINDOW) & (doc_col == 0)
    diff_new = pos_col - pos_row
    keep_new = (diff_new >= 0) & (diff_new < WINDOW) & (doc_col == doc_row)
    s_old = jnp.where(keep_old, lax.dot_general(q, kc, contract, preferred_element_type=F32) * SCORE_SCALE, NEG_BIG)
    s_new = jnp.where(keep_new, lax.dot_general(q, kn, contract, preferred_element_type=F32) * SCORE_SCALE, NEG_BIG)
    top = jnp.maximum(jnp.max(s_old, axis=-1, keepdims=True), jnp.max(s_new, axis=-1, keepdims=True))
    e_old = jnp.exp(s_old - top)
    e_new = jnp.exp(s_new - top)
    denom = jnp.sum(e_old, axis=-1, keepdims=True) + jnp.sum(e_new, axis=-1, keepdims=True)
    inv = 1.0 / denom
    out = jnp.dot((e_old * inv).astype(BF16), vc, preferred_element_type=F32) + jnp.dot((e_new * inv).astype(BF16), vn, preferred_element_type=F32)
    o_ref[...] = out.astype(BF16).astype(F32).reshape(o_ref.shape)
    window = kc.shape[0]
    target_row = lax.rem(pos_row, window)
    target_col = lax.rem(pos_col, window)
    hit = lax.broadcasted_iota(jnp.int32, (window, toks), 0) == target_row
    pick = jnp.where(hit, 1.0, 0.0)
    any_hit = jnp.max(pick, axis=1, keepdims=True) > 0.0
    pick = pick.astype(BF16)
    ko_ref[0] = jnp.where(any_hit, jnp.dot(pick, kn, preferred_element_type=F32), kc.astype(F32)).astype(BF16)
    vo_ref[0] = jnp.where(any_hit, jnp.dot(pick, vn, preferred_element_type=F32), vc.astype(F32)).astype(BF16)
    hit_t = lax.broadcasted_iota(jnp.int32, (toks, window), 1) == target_col
    newest = jnp.max(jnp.where(hit_t, pos_col, -1), axis=0, keepdims=True)
    so_ref[0] = jnp.where(newest >= 0, newest, slot)


def attn_call(q, k, v, k_cache, v_cache, slot_pos, seg_pos):
    seqs, toks = seg_pos.shape
    width = q.shape[-1]
    blocks = toks // 8
    window = k_cache.shape[1]
    shape4 = (blocks, seqs, 8, width)
    doc = jnp.cumsum((seg_pos == 0).astype(jnp.int32), axis=1)
    tok_spec = pl.BlockSpec((blocks, 1, 8, width), lambda s: (0, s, 0, 0))
    cache_spec = pl.BlockSpec((1, window, width), lambda s: (s, 0, 0))
    row_spec = lambda n: pl.BlockSpec((1, 1, n), lambda s: (s, 0, 0))
    col_spec = pl.BlockSpec((1, toks, 1), lambda s: (s, 0, 0))
    out, k_out, v_out, slot_out = pl.pallas_call(
        attn_kernel,
        grid=(seqs,),
        out_shape=(jax.ShapeDtypeStruct(shape4, F32), jax.ShapeDtypeStruct(k_cache.shape, BF16), jax.ShapeDtypeStruct(v_cache.shape, BF16), jax.ShapeDtypeStruct((seqs, 1, window), jnp.int32)),
        in_specs=[tok_spec, tok_spec, tok_spec, cache_spec, cache_spec, row_spec(window), row_spec(toks), col_spec, row_spec(toks), col_spec],
        out_specs=(tok_spec, cache_spec, cache_spec, row_spec(window)),
        cost_estimate=pl.CostEstimate(flops=8 * seqs * toks * window * width, bytes_accessed=8 * seqs * window * width, transcendentals=0),
        name='attention',
    )(q.reshape(shape4), k.reshape(shape4), v.reshape(shape4), k_cache, v_cache, slot_pos[:, None, :], seg_pos[:, None, :], seg_pos[:, :, None], doc[:, None, :], doc[:, :, None])
    return out.reshape(blocks * seqs * 8, width), k_out, v_out, slot_out.reshape(slot_pos.shape)


def solution(mesh):
    tp = mesh.shape['tp']

    def device_body(x_in, seg_pos, conv_state, lru_state, k_cache, v_cache, slot_pos, norm_scale, w_x, b_x, w_y, b_y, conv_w, conv_b, w_a, b_a, w_i, b_i, a_param, w_out, b_out, w_q, w_k, w_v, w_o, b_o, w_1, b_1, w_2, b_2, w_d, b_d):
        seqs, toks = seg_pos.shape
        dim = x_in.shape[-1]
        x = x_in.reshape(-1, dim)
        pos_col = seg_pos[:, :, None]
        soft = jax.nn.softplus(a_param)
        half = ROPE_DIM // 2
        timescale = 10000.0 ** (2.0 * jnp.arange(half).astype(F32) / ROPE_DIM)
        order = seg_pos.reshape(seqs, toks // 8, 8).swapaxes(0, 1).reshape(-1)
        angle = order[:, None].astype(F32) / timescale
        sin, cos = jnp.sin(angle), jnp.cos(angle)
        cos2 = jnp.concatenate([cos, cos], axis=1)
        sin2 = jnp.concatenate([-sin, sin], axis=1)

        def rec_post(layer):
            return ('rec', layer, norm_scale, (('p_x', w_x, layer), ('p_y', w_y, layer)), (('b_x', b_x), ('b_y', b_y)))

        def mlp_part(m):
            return (m, norm_scale, w_1, b_1, w_2, b_2, w_d, b_d)

        conv_list, lru_list = [], []
        out = comm_call(tp, 0, x, post=rec_post(0))
        for layer in range(2):
            mid, conv_new, lru_new = rec_call(layer, out['o_u'], out['o_y'], pos_col, conv_state, lru_state, conv_w, conv_b, w_a, b_a, w_i, b_i, soft)
            conv_list.append(conv_new)
            lru_list.append(lru_new)
            post = rec_post(1) if layer == 0 else ('attn', 0, norm_scale, (('p_q', w_q, None), ('p_k', w_k, None), ('p_v', w_v, None)), (('cos', cos2), ('sin', sin2)))
            out = comm_call(tp, layer + 1, x, pre=(mid.reshape(tp * x.shape[0], -1), layer, w_out, layer, b_out), mlp=mlp_part(layer), post=post)
            x = out['o_x']
        mid, k_out, v_out, slot_out = attn_call(out['o_q'], out['o_k'], out['o_v'], k_cache, v_cache, slot_pos, seg_pos)
        out = comm_call(tp, 3, x, pre=(mid, 0, w_o, None, b_o[None, :]), mlp=mlp_part(2))
        return out['o_x'].reshape(x_in.shape), jnp.stack(conv_list), jnp.stack(lru_list), k_out, v_out, slot_out

    col_spec = P(None, None, 'tp')
    vec_spec = P(None, 'tp')
    block_spec = P(None, 'tp', None, None)
    row_spec = P(None, 'tp', None)
    cache_spec = P('dp', None, None)
    arg_specs = (P('dp', 'tp', None), P('dp', None), P(None, 'dp', None, 'tp'), P(None, 'dp', 'tp'), cache_spec, cache_spec, P('dp', None), P(), col_spec, vec_spec, col_spec, vec_spec, col_spec, vec_spec, block_spec, vec_spec, block_spec, vec_spec, vec_spec, row_spec, P(), P(None, 'tp'), P(), P(), P('tp', None), P(), col_spec, vec_spec, col_spec, vec_spec, row_spec, P())
    result_specs = (P('dp', 'tp', None), P(None, 'dp', None, 'tp'), P(None, 'dp', 'tp'), cache_spec, cache_spec, P('dp', None))
    return jax.shard_map(device_body, mesh=mesh, in_specs=arg_specs, out_specs=result_specs, check_vma=False)
```

```python
import functools

import jax
import jax.numpy as jnp
from jax import lax
from jax.experimental import pallas as pl
from jax.experimental.pallas import tpu as pltpu
from jax.sharding import PartitionSpec as P

WINDOW = 2048
HEAD_DIM = 256
ROPE_DIM = 128
CONV_WIDTH = 4
SCORE_SCALE = 0.0625
NEG_BIG = -1e30
F32 = jnp.float32
BF16 = jnp.bfloat16

SLOT_REL = (0, -1, 1, -2, 2, -3, 3, 4)
ROW_TILE = 16


def slot_of(rel):
    if rel == 0:
        return 0
    if rel in (4, -4):
        return 7
    return -2 * rel - 1 if rel < 0 else 2 * rel


class Net:
    def __init__(self, tp, rows, dim, r):
        self.me = lax.axis_index('tp')
        self.core = lax.rem(self.me, 2)
        self.chips = tp // 2
        self.chip = lax.div(self.me, 2)
        self.up = lax.rem(self.me + 2, tp)
        self.down = lax.rem(self.me + tp - 2, tp)
        self.partner = self.me + 1 - 2 * self.core
        self.rows = rows
        self.groups = rows // ROW_TILE
        self.dim = dim
        self.cw = dim // 2
        self.r = r

    def barrier(self):
        sem = pltpu.get_barrier_semaphore()
        for other in (self.up, self.down, self.partner):
            pl.semaphore_signal(sem, inc=1, device_id={'tp': other}, device_id_type=pl.DeviceIdType.MESH)
        pl.semaphore_wait(sem, 3)

    def span(self, chunk):
        half, group = chunk
        cols = half * self.cw
        if not isinstance(half, int):
            cols = pl.multiple_of(cols, 128)
        return pl.ds(group * ROW_TILE, ROW_TILE), pl.ds(cols, self.cw)

    def remote(self, src, dst, send, recv, dev):
        return pltpu.make_async_remote_copy(src_ref=src, dst_ref=dst, send_sem=send, recv_sem=recv, device_id={'tp': dev}, device_id_type=pl.DeviceIdType.MESH)

    def ag_hop(self, way, d, chunk):
        sign = -1 if way == 0 else 1
        src, dst = slot_of(sign * (d - 1)), slot_of(sign * d)
        g, sems = self.r['g'], (way, d - 1) + chunk
        return self.remote(g.at[(2 * src + self.core,) + self.span(chunk)], g.at[(2 * dst + self.core,) + self.span(chunk)],
                           self.r['send_z'].at[sems], self.r['ag_z'].at[sems], self.up if way == 0 else self.down)

    def ag_pair(self, slot, chunk):
        ref, sems = self.r['g'].at[(2 * slot + self.core,) + self.span(chunk)], (slot,) + chunk
        return self.remote(ref, ref, self.r['send_d'].at[sems], self.r['ag_d'].at[sems], self.partner)

    def rs_pair(self, slot, chunk):
        idx, sems = (slot,) + self.span(chunk), (slot,) + chunk
        return self.remote(self.r['dsend'].at[idx], self.r['drecv'].at[idx], self.r['give_d'].at[sems], self.r['rs_d'].at[sems], self.partner)

    def rs_hop(self, way, d, chunk):
        idx, sems = (way, d - 1) + self.span(chunk), (way, d - 1) + chunk
        return self.remote(self.r['zsend'].at[idx], self.r['zrecv'].at[idx], self.r['give_z'].at[sems], self.r['rs_z'].at[sems], self.up if way == 0 else self.down)

    def chunks(self):
        return [(half, group) for group in range(self.groups) for half in range(2)]

    def hops(self):
        for way in range(2):
            for d in range(1, 5):
                for chunk in self.chunks():
                    if d < 4 or chunk[0] == way:
                        yield way, d, chunk

    def abs_chip(self, rel):
        return lax.rem(self.chip + (rel + self.chips), self.chips)

    def wait_pair(self, slots):
        for slot in slots:
            for chunk in self.chunks():
                self.ag_pair(slot, chunk).wait_recv()

    def gather_start(self, group):
        for k in range(2):
            self.ag_hop(0, 1, (k, group)).start()
            self.ag_hop(1, 1, (1 - k, group)).start()
        for k in range(2):
            self.ag_pair(0, (k, group)).start()

    def gather(self, run_pass):
        self.wait_pair((0,))
        run_pass(0, 1)
        for d in range(1, 5):
            for p in range(2 * self.groups if d < 4 else self.groups):
                for way in range(2):
                    chunk = ((p + way) % 2, p // 2) if d < 4 else (way, p)
                    self.ag_hop(way, d, chunk).wait_recv()
                    if d < 3 or (d == 3 and chunk[0] == way):
                        self.ag_hop(way, d + 1, chunk).start()
                    self.ag_pair(slot_of(-d if way == 0 else d), chunk).start()
                if p == 0 and d > 1:
                    self.wait_pair((2 * d - 3, 2 * d - 2))
                    run_pass(2 * d - 3, 2 * d - 1)

    def gather_end(self, run_pass):
        self.wait_pair((7,))
        run_pass(7, 8)
        for way, d, chunk in self.hops():
            self.ag_hop(way, d, chunk).wait_send()
        for slot in range(8):
            for chunk in self.chunks():
                self.ag_pair(slot, chunk).wait_send()

    def reduce(self, lhs_of, w_ref, finish, between=None):
        r, rows = self.r, self.rows
        sub = min(512, self.cw)
        steps = self.cw // sub

        def slots_of(d):
            return {4: (7,), 0: (0,)}.get(d, (slot_of(-d), slot_of(d)))

        def compute(d):
            slots = slots_of(d)
            for half in range(2):
                def body(t, carry):
                    span = pl.ds(pl.multiple_of(half * self.cw + t * sub, sub), sub)
                    lhs = jnp.concatenate([lhs_of(s, self.core) for s in slots] + [lhs_of(s, 1 - self.core) for s in slots], axis=0)
                    out = jnp.dot(lhs, w_ref[:, span], preferred_element_type=F32)
                    for i, s in enumerate(slots):
                        j = len(slots) + i
                        r['pown'][s, :, span] = out[i * rows:(i + 1) * rows]
                        r['dsend'][s, :, span] = out[j * rows:(j + 1) * rows].astype(BF16)
                    return carry
                lax.fori_loop(0, steps, body, 0)
                for group in range(self.groups):
                    for s in slots:
                        self.rs_pair(s, (half, group)).start()

        def combine(way, d, chunk):
            s = slot_of(d if way == 0 else -d)
            idx = self.span(chunk)
            self.rs_pair(s, chunk).wait_recv()
            total = r['pown'][(s,) + idx] + r['drecv'][(s,) + idx].astype(F32)
            if d < 3 or (d == 3 and chunk[0] == way):
                self.rs_hop(way, d + 1, chunk).wait_recv()
                total = total + r['zrecv'][(way, d) + idx].astype(F32)
            r['zsend'][(way, d - 1) + idx] = total.astype(BF16)
            self.rs_hop(way, d, chunk).start()

        def send(d, deep):
            for group in range(self.groups):
                for way in range(2):
                    combine(way, d, (way if deep else 1 - way, group))

        compute(3)
        send(3, False)
        compute(2)
        if between is not None:
            between()
        compute(4)
        send(2, False)
        send(4, True)
        compute(1)
        send(3, True)
        send(1, False)
        compute(0)
        send(2, True)
        send(1, True)
        for group in range(self.groups):
            for half in range(2):
                self.rs_pair(0, (half, group)).wait_recv()
                self.rs_hop(0, 1, (half, group)).wait_recv()
                self.rs_hop(1, 1, (half, group)).wait_recv()
                idx = self.span((half, group))
                total = r['pown'][(0,) + idx] + r['drecv'][(0,) + idx].astype(F32)
                total = total + r['zrecv'][(0, 0) + idx].astype(F32) + r['zrecv'][(1, 0) + idx].astype(F32)
                finish(idx, total)
            yield group

    def reduce_end(self):
        for way, d, chunk in self.hops():
            self.rs_hop(way, d, chunk).wait_send()
        for slot in range(8):
            for chunk in self.chunks():
                self.rs_pair(slot, chunk).wait_send()


def comm_kernel(cfg, names, outs, scratch, *refs):
    r = dict(zip(names + outs + scratch, refs))
    x_ref = r['x']
    rows, dim = x_ref.shape
    net = Net(cfg['tp'], rows, dim, r)
    loads = {}
    for i, (key, src, layer) in enumerate(cfg['loads']):
        view = r[src] if layer is None else r[src].at[layer]
        loads[key] = pltpu.make_async_copy(view, r[key], r['w_sem'].at[i])
        loads[key].start()
    net.barrier()
    xbuf = r['xbuf']
    xbuf[...] = x_ref[...]
    groups = range(net.groups)

    def normalize(idx, group):
        span = pl.ds(group * ROW_TILE, ROW_TILE)
        h = xbuf[span, :].astype(F32)
        inv = lax.rsqrt(jnp.mean(h * h, axis=-1, keepdims=True) + 1e-6)
        r['g'][net.core, span, :] = (h * inv * (1.0 + r['norm'][idx:idx + 1, :].astype(F32))).astype(BF16)

    def finish_with(bias_ref, idx):
        def finish(span, total):
            xbuf[span] = (xbuf[span].astype(F32) + total + bias_ref[idx:idx + 1, span[1]].astype(F32)).astype(BF16)
        return finish

    def block_of(first, last):
        return r['g'][2 * first:2 * last].reshape((last - first) * 2 * rows, dim)

    def enter(idx, steps=None):
        for group in groups if steps is None else steps:
            normalize(idx, group)
            net.gather_start(group)
        if steps is not None:
            net.reduce_end()

    reduction = None
    if cfg['pre'] is not None:
        r['apre'][...] = r['mid'][...].astype(BF16)
        loads['w_pre'].wait()

        def lhs_pre(slot, core):
            blk = 2 * net.abs_chip(SLOT_REL[slot]) + core
            return r['apre'][pl.ds(pl.multiple_of(blk * rows, 16), rows), :]
        reduction = net.reduce(lhs_pre, r['w_pre'], finish_with(r['b_pre'], cfg['pre']))

    if cfg['mlp'] is not None:
        m = cfg['mlp']
        pending = ['w_1s', 'w_2s', 'w_ds']

        def mlp_pass(first, last):
            while pending:
                loads[pending.pop()].wait()
            count = 2 * (last - first)

            def body(t, carry):
                cols = pl.ds(pl.multiple_of(t * 256, 256), 256)
                lhs = block_of(first, last)
                h1 = jnp.dot(lhs, r['w_1s'][:, cols], preferred_element_type=F32) + r['b_1'][m:m + 1, cols].astype(F32)
                h2 = jnp.dot(lhs, r['w_2s'][:, cols], preferred_element_type=F32) + r['b_2'][m:m + 1, cols].astype(F32)
                act = (jax.nn.gelu(h1, approximate=True) * h2).astype(BF16)
                r['act'][2 * first:2 * last, :, cols] = act.reshape(count, rows, 256)
                return carry
            lax.fori_loop(0, r['w_1s'].shape[1] // 256, body, 0)
        enter(2 * m + 1, reduction)
        net.gather(mlp_pass)
        reduction = net.reduce(lambda slot, core: r['act'][2 * slot + core], r['w_ds'], finish_with(r['b_d'], m), lambda: net.gather_end(mlp_pass))

    if cfg['post'] is not None:
        kind, idx = cfg['post']
        waiting = [key for key, _, _ in cfg['loads'] if key.startswith('p_')]

        def post_pass(first, last):
            while waiting:
                loads[waiting.pop()].wait()
            lhs = block_of(first, last)
            spans = [pl.ds(pl.multiple_of(net.abs_chip(SLOT_REL[s]) * 2 * rows, 16), 2 * rows) for s in range(first, last)]

            def put(ref, value, rope=False):
                for i, span in enumerate(spans):
                    v = value[i * 2 * rows:(i + 1) * 2 * rows]
                    if rope:
                        lo = v[:, :ROPE_DIM]
                        lo = lo * r['cos'][span, :] + pltpu.roll(lo, ROPE_DIM // 2, 1) * r['sin'][span, :]
                        v = jnp.concatenate([lo, v[:, ROPE_DIM:]], axis=1)
                    ref[span, :] = v.astype(BF16).astype(F32)
            if kind == 'rec':
                put(r['o_u'], jnp.dot(lhs, r['p_x'][...], preferred_element_type=F32) + r['b_x'][idx:idx + 1, :].astype(F32))
                put(r['o_y'], jax.nn.gelu(jnp.dot(lhs, r['p_y'][...], preferred_element_type=F32) + r['b_y'][idx:idx + 1, :].astype(F32), approximate=True))
            else:
                put(r['o_q'], jnp.dot(lhs, r['p_q'][...], preferred_element_type=F32), True)
                put(r['o_k'], jnp.dot(lhs, r['p_k'][...], preferred_element_type=F32), True)
                put(r['o_v'], jnp.dot(lhs, r['p_v'][...], preferred_element_type=F32))
        enter(4 if kind == 'attn' else 2 * idx, reduction)
        net.gather(post_pass)
        net.gather_end(post_pass)
    else:
        for _ in reduction:
            pass
        net.reduce_end()
    if 'o_x' in r:
        r['o_x'][...] = xbuf[...]


def comm_call(tp, ident, x, pre=None, mlp=None, post=None):
    rows, dim = x.shape
    vmem, hbm = pl.BlockSpec(memory_space=pltpu.VMEM), pl.BlockSpec(memory_space=pl.ANY)
    args, specs, names, loads, scratch = [], [], [], [], {}

    def add(name, value, spec):
        names.append(name)
        args.append(value)
        specs.append(spec)
    add('x', x, vmem)
    outs = {}
    flops = 0
    if pre is not None or mlp is not None:
        outs['o_x'] = jax.ShapeDtypeStruct((rows, dim), BF16)
        scratch['pown'] = pltpu.VMEM((8, rows, dim), F32)
        scratch['dsend'] = pltpu.VMEM((8, rows, dim), BF16)
        scratch['drecv'] = pltpu.VMEM((8, rows, dim), BF16)
        scratch['zsend'] = pltpu.VMEM((2, 4, rows, dim), BF16)
        scratch['zrecv'] = pltpu.VMEM((2, 4, rows, dim), BF16)
    if pre is not None:
        mid, b_idx, w_pre, layer, b_pre = pre
        add('mid', mid, vmem)
        add('h_pre', w_pre, hbm)
        add('b_pre', b_pre, vmem)
        loads.append(('w_pre', 'h_pre', layer))
        scratch['w_pre'] = pltpu.VMEM(w_pre.shape[-2:], BF16)
        scratch['apre'] = pltpu.VMEM(mid.shape, BF16)
        flops += 2 * mid.shape[0] * w_pre.shape[-2] * dim
    if mlp is not None:
        m, norm, w_1, b_1, w_2, b_2, w_d, b_d = mlp
        ff = w_1.shape[-1]
        for key, value in (('h_1', w_1), ('h_2', w_2), ('h_d', w_d)):
            add(key, value, hbm)
        for key, value in (('b_1', b_1), ('b_2', b_2), ('b_d', b_d)):
            add(key, value, vmem)
        loads += [('w_1s', 'h_1', m), ('w_2s', 'h_2', m), ('w_ds', 'h_d', m)]
        scratch['w_1s'] = pltpu.VMEM((dim, ff), BF16)
        scratch['w_2s'] = pltpu.VMEM((dim, ff), BF16)
        scratch['w_ds'] = pltpu.VMEM((ff, dim), BF16)
        scratch['act'] = pltpu.VMEM((tp, rows, ff), BF16)
        flops += 6 * tp * rows * ff * dim
    else:
        norm = post[2]
    add('norm', norm, vmem)
    if post is not None:
        kind, idx, _, weights, extras = post
        width = weights[0][1].shape[-1]
        for key, value, layer in weights:
            add('h_' + key, value, hbm)
            loads.append((key, 'h_' + key, layer))
            scratch[key] = pltpu.VMEM(value.shape[-2:], BF16)
            outs['o_' + key[2:] if kind == 'attn' else {'p_x': 'o_u', 'p_y': 'o_y'}[key]] = jax.ShapeDtypeStruct((tp * rows, width), F32)
            flops += 2 * tp * rows * dim * width
        for key, value in extras:
            add(key, value, vmem)
    scratch['g'] = pltpu.VMEM((tp, rows, dim), BF16)
    scratch['xbuf'] = pltpu.VMEM((rows, dim), BF16)
    for key in ('ag_z', 'rs_z', 'send_z', 'give_z'):
        scratch[key] = pltpu.SemaphoreType.DMA((2, 4, 2, rows // ROW_TILE))
    for key in ('ag_d', 'rs_d', 'send_d', 'give_d'):
        scratch[key] = pltpu.SemaphoreType.DMA((8, 2, rows // ROW_TILE))
    scratch['w_sem'] = pltpu.SemaphoreType.DMA((len(loads),))
    cfg = dict(tp=tp, loads=tuple(loads), pre=None if pre is None else pre[1], mlp=None if mlp is None else mlp[0],
               post=None if post is None else (post[0], post[1]))
    result = pl.pallas_call(
        functools.partial(comm_kernel, cfg, names, list(outs), list(scratch)),
        out_shape=tuple(outs.values()),
        in_specs=specs,
        out_specs=tuple(vmem for _ in outs),
        scratch_shapes=list(scratch.values()),
        compiler_params=pltpu.CompilerParams(collective_id=ident, has_side_effects=True, vmem_limit_bytes=66 * 1000 * 1000),
        cost_estimate=pl.CostEstimate(flops=flops, bytes_accessed=flops // 1500, transcendentals=0),
        name='ring_' + str(ident),
    )(*args)
    return dict(zip(outs, result))


def column_of(row):
    n = row.shape[1]
    return jnp.broadcast_to(row, (n, n)).T[:, :1]


def rec_kernel(layer, seqs, u_ref, y_ref, pos_ref, cs_ref, ls_ref, cw_ref, cb_ref, wa_ref, ba_ref, wi_ref, bi_ref, sp_ref, hy_ref, co_ref, lo_ref, pad):
    blocks = u_ref.shape[0]
    toks = blocks * 8
    width = u_ref.shape[-1]

    def one_seq(s, carry):
        u = u_ref[:, s].reshape(toks, width)
        pad[8:8 + toks, :] = u
        pad[5:8, :] = cs_ref[s].astype(F32)
        co_ref[s] = u[toks - 3:, :].astype(BF16)
        total = jnp.zeros((toks, width), F32)
        for j in range(CONV_WIDTH):
            total = total + pad[5 + j:5 + j + toks, :] * cw_ref[layer, j:j + 1, :].astype(F32)
        conv = (total + cb_ref[layer:layer + 1, :].astype(F32)).astype(BF16)
        gate_r = jax.nn.sigmoid(jnp.dot(conv, wa_ref[0], preferred_element_type=F32) + ba_ref[layer:layer + 1, :].astype(F32))
        gate_i = jax.nn.sigmoid(jnp.dot(conv, wi_ref[0], preferred_element_type=F32) + bi_ref[layer:layer + 1, :].astype(F32))
        decay = jnp.exp(-8.0 * gate_r * sp_ref[layer:layer + 1, :])
        reset = column_of(pos_ref[pl.ds(s, 1), :]) == 0
        mult = jnp.where(reset, 1.0, jnp.sqrt(1.0 - decay * decay))
        decay = jnp.where(reset, 0.0, decay)
        drive = conv.astype(F32) * gate_i * mult
        a = decay.reshape(blocks, 8, width)
        b = drive.reshape(blocks, 8, width)
        row = lax.broadcasted_iota(jnp.int32, (blocks, 8, width), 1)
        for k in (1, 2, 4):
            inside = row >= k
            a_sh = jnp.where(inside, pltpu.roll(a, k, 1), 1.0)
            b_sh = jnp.where(inside, pltpu.roll(b, k, 1), 0.0)
            b = a * b_sh + b
            a = a * a_sh
        state = ls_ref[pl.ds(s, 1), :]
        for blk in range(blocks):
            h = a[blk] * state + b[blk]
            state = h[7:8, :]
            hy_ref[blk, s] = (h * y_ref[blk, s]).astype(BF16).astype(F32)
        lo_ref[pl.ds(s, 1), :] = state
        return carry
    lax.fori_loop(0, seqs, one_seq, 0)


def rec_call(layer, u, y, seg_pos, conv_state, lru_state, conv_w, conv_b, w_a, b_a, w_i, b_i, soft):
    seqs, toks = seg_pos.shape
    width = u.shape[-1]
    blocks = toks // 8
    shape4 = (blocks, seqs, 8, width)
    full = pl.BlockSpec(memory_space=pltpu.VMEM)
    layer_spec = lambda a: pl.BlockSpec((None,) + a.shape[1:], functools.partial(lambda n, i: (layer,) + (0,) * n, a.ndim - 1))
    whole = lambda a: pl.BlockSpec(a.shape, functools.partial(lambda n, i: (0,) * n, a.ndim))
    out_shape = (jax.ShapeDtypeStruct(shape4, F32), jax.ShapeDtypeStruct((seqs, 3, width), BF16), jax.ShapeDtypeStruct((seqs, width), F32))
    args = (u.reshape(shape4), y.reshape(shape4), seg_pos, conv_state, lru_state, conv_w, conv_b, w_a, b_a, w_i, b_i, soft)
    per_layer = {3, 4, 7, 9}
    return pl.pallas_call(
        functools.partial(rec_kernel, layer, seqs),
        grid=(1,),
        out_shape=out_shape,
        in_specs=[layer_spec(a) if i in per_layer else whole(a) for i, a in enumerate(args)],
        out_specs=tuple(whole(a) for a in out_shape),
        scratch_shapes=[pltpu.VMEM((toks + 8, width), F32)],
        cost_estimate=pl.CostEstimate(flops=4 * toks * seqs * width * width, bytes_accessed=16 * toks * seqs * width, transcendentals=0),
        name='recurrence_' + str(layer),
    )(*args)


def attn_kernel(q_ref, k_ref, v_ref, kc_ref, vc_ref, slot_ref, pos_ref, o_ref, ko_ref, vo_ref, so_ref):
    blocks, _, _, width = q_ref.shape
    toks = blocks * 8
    q = q_ref[...].reshape(toks, width).astype(BF16)
    kn = k_ref[...].reshape(toks, width).astype(BF16)
    vn = v_ref[...].reshape(toks, width).astype(BF16)
    kc, vc = kc_ref[0], vc_ref[0]
    seq = pl.ds(pl.program_id(0), 1)
    slot, pos_row = slot_ref[seq, :], pos_ref[seq, :]
    pos_mat = jnp.broadcast_to(pos_row, (toks, toks))
    pos_mat_t = pos_mat.T
    pos_col = pos_mat_t[:, :1]
    row_i = lax.broadcasted_iota(jnp.int32, (toks, toks), 0)
    col_i = lax.broadcasted_iota(jnp.int32, (toks, toks), 1)
    doc_col = jnp.sum(jnp.where((pos_mat == 0) & (col_i <= row_i), 1.0, 0.0), axis=1, keepdims=True)
    doc_row = jnp.sum(jnp.where((pos_mat_t == 0) & (row_i <= col_i), 1.0, 0.0), axis=0, keepdims=True)
    contract = (((1,), (1,)), ((), ()))
    diff_old = pos_col - slot
    keep_old = (slot >= 0) & (diff_old >= 0) & (diff_old < WINDOW) & (doc_col == 0)
    diff_new = pos_col - pos_row
    keep_new = (diff_new >= 0) & (diff_new < WINDOW) & (doc_col == doc_row)
    s_old = jnp.where(keep_old, lax.dot_general(q, kc, contract, preferred_element_type=F32) * SCORE_SCALE, NEG_BIG)
    s_new = jnp.where(keep_new, lax.dot_general(q, kn, contract, preferred_element_type=F32) * SCORE_SCALE, NEG_BIG)
    top = jnp.maximum(jnp.max(s_old, axis=-1, keepdims=True), jnp.max(s_new, axis=-1, keepdims=True))
    e_old = jnp.exp(s_old - top)
    e_new = jnp.exp(s_new - top)
    denom = jnp.sum(e_old, axis=-1, keepdims=True) + jnp.sum(e_new, axis=-1, keepdims=True)
    inv = 1.0 / denom
    out = jnp.dot((e_old * inv).astype(BF16), vc, preferred_element_type=F32) + jnp.dot((e_new * inv).astype(BF16), vn, preferred_element_type=F32)
    o_ref[...] = out.astype(BF16).astype(F32).reshape(o_ref.shape)
    window = kc.shape[0]
    target_row = lax.rem(pos_row, window)
    target_col = lax.rem(pos_col, window)
    hit = lax.broadcasted_iota(jnp.int32, (window, toks), 0) == target_row
    pick = jnp.where(hit, 1.0, 0.0)
    any_hit = jnp.max(pick, axis=1, keepdims=True) > 0.0
    pick = pick.astype(BF16)
    ko_ref[0] = jnp.where(any_hit, jnp.dot(pick, kn, preferred_element_type=F32), kc.astype(F32)).astype(BF16)
    vo_ref[0] = jnp.where(any_hit, jnp.dot(pick, vn, preferred_element_type=F32), vc.astype(F32)).astype(BF16)
    hit_t = lax.broadcasted_iota(jnp.int32, (toks, window), 1) == target_col
    newest = jnp.max(jnp.where(hit_t, pos_col, -1), axis=0, keepdims=True)
    so_ref[seq, :] = jnp.where(newest >= 0, newest, slot)


def attn_call(q, k, v, k_cache, v_cache, slot_pos, seg_pos):
    seqs, toks = seg_pos.shape
    width = q.shape[-1]
    blocks = toks // 8
    window = k_cache.shape[1]
    shape4 = (blocks, seqs, 8, width)
    tok_spec = pl.BlockSpec((blocks, 1, 8, width), lambda s: (0, s, 0, 0))
    cache_spec = pl.BlockSpec((1, window, width), lambda s: (s, 0, 0))
    row_spec = lambda n: pl.BlockSpec((seqs, n), lambda s: (0, 0))
    out, k_out, v_out, slot_out = pl.pallas_call(
        attn_kernel,
        grid=(seqs,),
        out_shape=(jax.ShapeDtypeStruct(shape4, F32), jax.ShapeDtypeStruct(k_cache.shape, BF16), jax.ShapeDtypeStruct(v_cache.shape, BF16), jax.ShapeDtypeStruct((seqs, window), jnp.int32)),
        in_specs=[tok_spec, tok_spec, tok_spec, cache_spec, cache_spec, row_spec(window), row_spec(toks)],
        out_specs=(tok_spec, cache_spec, cache_spec, row_spec(window)),
        cost_estimate=pl.CostEstimate(flops=8 * seqs * toks * window * width, bytes_accessed=8 * seqs * window * width, transcendentals=0),
        name='attention',
    )(q.reshape(shape4), k.reshape(shape4), v.reshape(shape4), k_cache, v_cache, slot_pos, seg_pos)
    return out.reshape(blocks * seqs * 8, width), k_out, v_out, slot_out


def solution(mesh):
    tp = mesh.shape['tp']

    def device_body(x_in, seg_pos, conv_state, lru_state, k_cache, v_cache, slot_pos, norm_scale, w_x, b_x, w_y, b_y, conv_w, conv_b, w_a, b_a, w_i, b_i, a_param, w_out, b_out, w_q, w_k, w_v, w_o, b_o, w_1, b_1, w_2, b_2, w_d, b_d):
        seqs, toks = seg_pos.shape
        dim = x_in.shape[-1]
        x = x_in.reshape(-1, dim)
        soft = jax.nn.softplus(a_param)
        half = ROPE_DIM // 2
        timescale = 10000.0 ** (2.0 * jnp.arange(half).astype(F32) / ROPE_DIM)
        order = seg_pos.reshape(seqs, toks // 8, 8).swapaxes(0, 1).reshape(-1)
        angle = order[:, None].astype(F32) / timescale
        sin, cos = jnp.sin(angle), jnp.cos(angle)
        cos2 = jnp.concatenate([cos, cos], axis=1)
        sin2 = jnp.concatenate([-sin, sin], axis=1)

        def rec_post(layer):
            return ('rec', layer, norm_scale, (('p_x', w_x, layer), ('p_y', w_y, layer)), (('b_x', b_x), ('b_y', b_y)))

        def mlp_part(m):
            return (m, norm_scale, w_1, b_1, w_2, b_2, w_d, b_d)

        conv_list, lru_list = [], []
        out = comm_call(tp, 0, x, post=rec_post(0))
        for layer in range(2):
            mid, conv_new, lru_new = rec_call(layer, out['o_u'], out['o_y'], seg_pos, conv_state, lru_state, conv_w, conv_b, w_a, b_a, w_i, b_i, soft)
            conv_list.append(conv_new)
            lru_list.append(lru_new)
            post = rec_post(1) if layer == 0 else ('attn', 0, norm_scale, (('p_q', w_q, None), ('p_k', w_k, None), ('p_v', w_v, None)), (('cos', cos2), ('sin', sin2)))
            out = comm_call(tp, layer + 1, x, pre=(mid.reshape(tp * x.shape[0], -1), layer, w_out, layer, b_out), mlp=mlp_part(layer), post=post)
            x = out['o_x']
        mid, k_out, v_out, slot_out = attn_call(out['o_q'], out['o_k'], out['o_v'], k_cache, v_cache, slot_pos, seg_pos)
        out = comm_call(tp, 3, x, pre=(mid, 0, w_o, None, b_o[None, :]), mlp=mlp_part(2))
        return out['o_x'].reshape(x_in.shape), jnp.stack(conv_list), jnp.stack(lru_list), k_out, v_out, slot_out

    col_spec = P(None, None, 'tp')
    vec_spec = P(None, 'tp')
    block_spec = P(None, 'tp', None, None)
    row_spec = P(None, 'tp', None)
    cache_spec = P('dp', None, None)
    arg_specs = (P('dp', 'tp', None), P('dp', None), P(None, 'dp', None, 'tp'), P(None, 'dp', 'tp'), cache_spec, cache_spec, P('dp', None), P(), col_spec, vec_spec, col_spec, vec_spec, col_spec, vec_spec, block_spec, vec_spec, block_spec, vec_spec, vec_spec, row_spec, P(), P(None, 'tp'), P(), P(), P('tp', None), P(), col_spec, vec_spec, col_spec, vec_spec, row_spec, P())
    result_specs = (P('dp', 'tp', None), P(None, 'dp', None, 'tp'), P(None, 'dp', 'tp'), cache_spec, cache_spec, P('dp', None))
    return jax.shard_map(device_body, mesh=mesh, in_specs=arg_specs, out_specs=result_specs, check_vma=False)
```

```python
import functools

import jax
import jax.numpy as jnp
from jax import lax
from jax.experimental import pallas as pl
from jax.experimental.pallas import tpu as pltpu
from jax.sharding import PartitionSpec as P

WINDOW = 2048
HEAD_DIM = 256
ROPE_DIM = 128
CONV_WIDTH = 4
SCORE_SCALE = 0.0625
NEG_BIG = -1e30
F32 = jnp.float32
BF16 = jnp.bfloat16

SLOT_REL = (0, -1, 1, -2, 2, -3, 3, 4)
ROW_TILE = 16


def slot_of(rel):
    if rel == 0:
        return 0
    if rel in (4, -4):
        return 7
    return -2 * rel - 1 if rel < 0 else 2 * rel


class Net:
    def __init__(self, tp, rows, dim, r):
        self.me = lax.axis_index('tp')
        self.core = lax.rem(self.me, 2)
        self.chips = tp // 2
        self.chip = lax.div(self.me, 2)
        self.up = lax.rem(self.me + 2, tp)
        self.down = lax.rem(self.me + tp - 2, tp)
        self.partner = self.me + 1 - 2 * self.core
        self.rows = rows
        self.groups = rows // ROW_TILE
        self.dim = dim
        self.cw = dim // 2
        self.r = r

    def barrier(self):
        sem = pltpu.get_barrier_semaphore()
        for other in (self.up, self.down, self.partner):
            pl.semaphore_signal(sem, inc=1, device_id={'tp': other}, device_id_type=pl.DeviceIdType.MESH)
        pl.semaphore_wait(sem, 3)

    def span(self, chunk):
        half, group = chunk
        cols = half * self.cw
        if not isinstance(half, int):
            cols = pl.multiple_of(cols, 128)
        return pl.ds(group * ROW_TILE, ROW_TILE), pl.ds(cols, self.cw)

    def remote(self, src, dst, send, recv, dev):
        return pltpu.make_async_remote_copy(src_ref=src, dst_ref=dst, send_sem=send, recv_sem=recv, device_id={'tp': dev}, device_id_type=pl.DeviceIdType.MESH)

    def ag_hop(self, way, d, chunk):
        sign = -1 if way == 0 else 1
        src, dst = slot_of(sign * (d - 1)), slot_of(sign * d)
        g, sems = self.r['g'], (way, d - 1) + chunk
        return self.remote(g.at[(2 * src + self.core,) + self.span(chunk)], g.at[(2 * dst + self.core,) + self.span(chunk)],
                           self.r['send_z'].at[sems], self.r['ag_z'].at[sems], self.up if way == 0 else self.down)

    def ag_pair(self, slot, chunk):
        ref, sems = self.r['g'].at[(2 * slot + self.core,) + self.span(chunk)], (slot,) + chunk
        return self.remote(ref, ref, self.r['send_d'].at[sems], self.r['ag_d'].at[sems], self.partner)

    def rs_pair(self, slot, chunk):
        idx, sems = (slot,) + self.span(chunk), (slot,) + chunk
        return self.remote(self.r['dsend'].at[idx], self.r['drecv'].at[idx], self.r['give_d'].at[sems], self.r['rs_d'].at[sems], self.partner)

    def rs_hop(self, way, d, chunk):
        idx, sems = (way, d - 1) + self.span(chunk), (way, d - 1) + chunk
        return self.remote(self.r['zsend'].at[idx], self.r['zrecv'].at[idx], self.r['give_z'].at[sems], self.r['rs_z'].at[sems], self.up if way == 0 else self.down)

    def chunks(self):
        return [(half, group) for group in range(self.groups) for half in range(2)]

    def hops(self):
        for way in range(2):
            for d in range(1, 5):
                for chunk in self.chunks():
                    if d < 4 or chunk[0] == way:
                        yield way, d, chunk

    def abs_chip(self, rel):
        return lax.rem(self.chip + (rel + self.chips), self.chips)

    def wait_pair(self, slots):
        for slot in slots:
            for chunk in self.chunks():
                self.ag_pair(slot, chunk).wait_recv()

    def gather_start(self, group):
        for k in range(2):
            self.ag_hop(0, 1, (k, group)).start()
            self.ag_hop(1, 1, (1 - k, group)).start()
        for k in range(2):
            self.ag_pair(0, (k, group)).start()

    def gather(self, run_pass):
        for d in range(1, 5):
            for p in range(2 * self.groups if d < 4 else self.groups):
                for way in range(2):
                    chunk = ((p + way) % 2, p // 2) if d < 4 else (way, p)
                    self.ag_hop(way, d, chunk).wait_recv()
                    if d < 3 or (d == 3 and chunk[0] == way):
                        self.ag_hop(way, d + 1, chunk).start()
                    self.ag_pair(slot_of(-d if way == 0 else d), chunk).start()
                if p == 0 and d > 1:
                    first = 0 if d == 2 else 2 * d - 3
                    self.wait_pair(range(first, 2 * d - 1))
                    run_pass(first, 2 * d - 1)

    def gather_end(self, run_pass):
        self.wait_pair((7,))
        run_pass(7, 8)
        for way, d, chunk in self.hops():
            self.ag_hop(way, d, chunk).wait_send()
        for slot in range(8):
            for chunk in self.chunks():
                self.ag_pair(slot, chunk).wait_send()

    def reduce(self, lhs_of, w_ref, finish, between=None):
        r, rows = self.r, self.rows
        sub = min(512, self.cw)
        steps = self.cw // sub

        def slots_of(d):
            return {4: (7,), 0: (0,)}.get(d, (slot_of(-d), slot_of(d)))

        def compute(d):
            slots = slots_of(d)
            for half in range(2):
                def body(t, carry):
                    span = pl.ds(pl.multiple_of(half * self.cw + t * sub, sub), sub)
                    lhs = jnp.concatenate([lhs_of(s, self.core) for s in slots] + [lhs_of(s, 1 - self.core) for s in slots], axis=0)
                    out = jnp.dot(lhs, w_ref[:, span], preferred_element_type=F32)
                    for i, s in enumerate(slots):
                        j = len(slots) + i
                        r['pown'][s, :, span] = out[i * rows:(i + 1) * rows]
                        r['dsend'][s, :, span] = out[j * rows:(j + 1) * rows].astype(BF16)
                    return carry
                lax.fori_loop(0, steps, body, 0)
                for group in range(self.groups):
                    for s in slots:
                        self.rs_pair(s, (half, group)).start()

        def combine(way, d, chunk):
            s = slot_of(d if way == 0 else -d)
            idx = self.span(chunk)
            self.rs_pair(s, chunk).wait_recv()
            total = r['pown'][(s,) + idx] + r['drecv'][(s,) + idx].astype(F32)
            if d < 3 or (d == 3 and chunk[0] == way):
                self.rs_hop(way, d + 1, chunk).wait_recv()
                total = total + r['zrecv'][(way, d) + idx].astype(F32)
            r['zsend'][(way, d - 1) + idx] = total.astype(BF16)
            self.rs_hop(way, d, chunk).start()

        def send(d, deep):
            for group in range(self.groups):
                for way in range(2):
                    combine(way, d, (way if deep else 1 - way, group))

        compute(3)
        send(3, False)
        compute(2)
        if between is not None:
            between()
        compute(4)
        send(2, False)
        send(4, True)
        compute(1)
        send(3, True)
        send(1, False)
        compute(0)
        send(2, True)
        send(1, True)
        for group in range(self.groups):
            for half in range(2):
                self.rs_pair(0, (half, group)).wait_recv()
                self.rs_hop(0, 1, (half, group)).wait_recv()
                self.rs_hop(1, 1, (half, group)).wait_recv()
                idx = self.span((half, group))
                total = r['pown'][(0,) + idx] + r['drecv'][(0,) + idx].astype(F32)
                total = total + r['zrecv'][(0, 0) + idx].astype(F32) + r['zrecv'][(1, 0) + idx].astype(F32)
                finish(idx, total)
            yield group

    def reduce_end(self):
        for way, d, chunk in self.hops():
            self.rs_hop(way, d, chunk).wait_send()
        for slot in range(8):
            for chunk in self.chunks():
                self.rs_pair(slot, chunk).wait_send()


def recurrence(layer, r):
    u_ref, y_ref, pad = r['u'], r['y'], r['pad']
    blocks, seqs, _, width = u_ref.shape
    toks = blocks * 8

    def one_seq(s, carry):
        u = u_ref[:, s].reshape(toks, width)
        pad[8:8 + toks, :] = u
        pad[5:8, :] = r['conv_state'][layer, s].astype(F32)
        r['o_conv'][s] = u[toks - 3:, :].astype(BF16)
        total = jnp.zeros((toks, width), F32)
        for j in range(CONV_WIDTH):
            total = total + pad[5 + j:5 + j + toks, :] * r['conv_w'][layer, j:j + 1, :].astype(F32)
        row_of = lambda key: r[key][layer:layer + 1, :].astype(F32)
        conv = (total + row_of('conv_b')).astype(BF16)
        gate_r = jax.nn.sigmoid(jnp.dot(conv, r['w_a'][layer, 0], preferred_element_type=F32) + row_of('b_a'))
        gate_i = jax.nn.sigmoid(jnp.dot(conv, r['w_i'][layer, 0], preferred_element_type=F32) + row_of('b_i'))
        decay = jnp.exp(-8.0 * gate_r * row_of('soft'))
        reset = r['reset'][s]
        mult = reset + (1.0 - reset) * jnp.sqrt(1.0 - decay * decay)
        decay = decay * (1.0 - reset)
        drive = conv.astype(F32) * gate_i * mult
        a = decay.reshape(blocks, 8, width)
        b = drive.reshape(blocks, 8, width)
        for k in (1, 2, 4):
            inside = r['inside'][k // 2]
            a_sh = pltpu.roll(a, k, 1) * inside + (1.0 - inside)
            b_sh = pltpu.roll(b, k, 1) * inside
            b = a * b_sh + b
            a = a * a_sh
        state = r['lru_state'][layer, pl.ds(s, 1), :]
        for blk in range(blocks):
            h = a[blk] * state + b[blk]
            state = h[7:8, :]
            u_ref[blk, s] = h * y_ref[blk, s]
        r['o_lru'][pl.ds(s, 1), :] = state
        return carry
    lax.fori_loop(0, seqs, one_seq, 0)


def comm_kernel(plan, tp, names, outs, scratch, *refs):
    r = dict(zip(names + outs + scratch, refs))
    x_ref = r['x']
    rows, dim = x_ref.shape
    net = Net(tp, rows, dim, r)
    loads = [[] for _ in plan]
    count = 0
    for i, step in enumerate(plan):
        for key, src, layer in step['loads']:
            view = r[src] if layer is None else r[src].at[layer]
            loads[i].append((key, pltpu.make_async_copy(view, r[key], r['w_sem'].at[count])))
            count += 1
    used = set()
    for step in loads:
        for key, copy in step:
            if key not in used:
                used.add(key)
                copy.start()

    def refill(i):
        for key, _ in loads[i]:
            later = [copy for step in loads[i + 1:] for k, copy in step if k == key]
            if later:
                later[0].start()

    net.barrier()
    xbuf = r['xbuf']
    xbuf[...] = x_ref[...]
    groups = range(net.groups)

    def enter(idx, steps):
        for group in groups if steps is None else steps:
            span = pl.ds(group * ROW_TILE, ROW_TILE)
            h = xbuf[span, :].astype(F32)
            inv = lax.rsqrt(jnp.mean(h * h, axis=-1, keepdims=True) + 1e-6)
            r['g'][net.core, span, :] = (h * inv * (1.0 + r['norm'][idx:idx + 1, :].astype(F32))).astype(BF16)
            net.gather_start(group)
        if steps is not None:
            net.reduce_end()

    def finish_with(bias_ref, idx):
        def finish(span, total):
            xbuf[span] = (xbuf[span].astype(F32) + total + bias_ref[idx:idx + 1, span[1]].astype(F32)).astype(BF16)
        return finish

    def block_of(first, last):
        return r['g'][2 * first:2 * last].reshape((last - first) * 2 * rows, dim)

    def wait_loads(i):
        pending = list(loads[i])

        def wait():
            while pending:
                pending.pop()[1].wait()
        return wait

    reduction = None
    for i, step in enumerate(plan):
        kind, idx = step['kind'], step['idx']
        ready = wait_loads(i)
        if kind == 'pre':
            ready()
            source = r['mid'] if 'mid' in r else r['u']
            r['apre'][...] = source[...].reshape(r['apre'].shape).astype(BF16)

            def lhs_pre(slot, core):
                blk = 2 * net.abs_chip(SLOT_REL[slot]) + core
                return r['apre'][pl.ds(pl.multiple_of(blk * rows, 16), rows), :]
            reduction = net.reduce(lhs_pre, r['w_pre'], finish_with(r['b_pre'], idx))
            owner = i
        elif kind == 'mlp':
            def mlp_pass(first, last, ready=ready, m=idx):
                ready()
                width = 2 * (last - first)

                def body(t, carry):
                    cols = pl.ds(pl.multiple_of(t * 256, 256), 256)
                    lhs = block_of(first, last)
                    h1 = jnp.dot(lhs, r['w_1s'][:, cols], preferred_element_type=F32) + r['b_1'][m:m + 1, cols].astype(F32)
                    h2 = jnp.dot(lhs, r['w_2s'][:, cols], preferred_element_type=F32) + r['b_2'][m:m + 1, cols].astype(F32)
                    act = (jax.nn.gelu(h1, approximate=True) * h2).astype(BF16)
                    r['act'][2 * first:2 * last, :, cols] = act.reshape(width, rows, 256)
                    return carry
                lax.fori_loop(0, r['w_1s'].shape[1] // 256, body, 0)
            enter(2 * idx + 1, reduction)
            refill(owner)
            net.gather(mlp_pass)
            reduction = net.reduce(lambda slot, core: r['act'][2 * slot + core], r['w_ds'], finish_with(r['b_d'], idx), functools.partial(net.gather_end, mlp_pass))
            owner = i
        else:
            def post_pass(first, last, ready=ready, kind=kind, layer=idx):
                ready()
                lhs = block_of(first, last)
                chips = [net.abs_chip(SLOT_REL[s]) for s in range(first, last)]

                def put(ref, value, rope=False):
                    for n, chip in enumerate(chips):
                        v = value[n * 2 * rows:(n + 1) * 2 * rows]
                        if rope:
                            span = pl.ds(pl.multiple_of(chip * 2 * rows, 16), 2 * rows)
                            lo = v[:, :ROPE_DIM]
                            lo = lo * r['cos'][span, :] + pltpu.roll(lo, ROPE_DIM // 2, 1) * r['sin'][span, :]
                            v = jnp.concatenate([lo, v[:, ROPE_DIM:]], axis=1)
                        ref[pl.ds(2 * chip, 2)] = v.astype(BF16).astype(F32).reshape((2,) + ref.shape[1:])
                if kind == 'rec':
                    put(r['u'], jnp.dot(lhs, r['p_0'][...], preferred_element_type=F32) + r['b_x'][layer:layer + 1, :].astype(F32))
                    put(r['y'], jax.nn.gelu(jnp.dot(lhs, r['p_1'][...], preferred_element_type=F32) + r['b_y'][layer:layer + 1, :].astype(F32), approximate=True))
                else:
                    put(r['o_q'], jnp.dot(lhs, r['p_0'][...], preferred_element_type=F32), True)
                    put(r['o_k'], jnp.dot(lhs, r['p_1'][...], preferred_element_type=F32), True)
                    put(r['o_v'], jnp.dot(lhs, r['p_2'][...], preferred_element_type=F32))
            enter(4 if kind == 'attn' else 2 * idx, reduction)
            if reduction is not None:
                refill(owner)
            net.gather(post_pass)
            net.gather_end(post_pass)
            refill(i)
            reduction = None
            if kind == 'rec':
                recurrence(idx, r)
    if reduction is not None:
        for _ in reduction:
            pass
        net.reduce_end()
    r['o_x'][...] = xbuf[...]


def comm_call(tp, ident, x, plan, small, large, outs, extra):
    rows, dim = x.shape
    vmem, hbm = pl.BlockSpec(memory_space=pltpu.VMEM), pl.BlockSpec(memory_space=pl.ANY)
    small = dict(x=x, **small)
    names = list(small) + list(large)
    outs = dict(o_x=jax.ShapeDtypeStruct((rows, dim), BF16), **outs)
    scratch = dict(extra)
    flops = 0
    total = 0
    for step in plan:
        for key, src, layer in step['loads']:
            shape = large[src].shape[-2:]
            scratch.setdefault(key, pltpu.VMEM(shape, BF16))
            flops += 2 * tp * rows * shape[0] * shape[1]
            total += 1
    scratch['pown'] = pltpu.VMEM((8, rows, dim), F32)
    scratch['dsend'] = pltpu.VMEM((8, rows, dim), BF16)
    scratch['drecv'] = pltpu.VMEM((8, rows, dim), BF16)
    scratch['zsend'] = pltpu.VMEM((2, 4, rows, dim), BF16)
    scratch['zrecv'] = pltpu.VMEM((2, 4, rows, dim), BF16)
    scratch['act'] = pltpu.VMEM((tp, rows, scratch['w_1s'].shape[1]), BF16)
    scratch['apre'] = pltpu.VMEM((tp * rows, scratch['w_pre'].shape[0]), BF16)
    scratch['g'] = pltpu.VMEM((tp, rows, dim), BF16)
    scratch['xbuf'] = pltpu.VMEM((rows, dim), BF16)
    for key in ('ag_z', 'rs_z', 'send_z', 'give_z'):
        scratch[key] = pltpu.SemaphoreType.DMA((2, 4, 2, rows // ROW_TILE))
    for key in ('ag_d', 'rs_d', 'send_d', 'give_d'):
        scratch[key] = pltpu.SemaphoreType.DMA((8, 2, rows // ROW_TILE))
    scratch['w_sem'] = pltpu.SemaphoreType.DMA((total,))
    result = pl.pallas_call(
        functools.partial(comm_kernel, plan, tp, names, list(outs), list(scratch)),
        out_shape=tuple(outs.values()),
        in_specs=[vmem] * len(small) + [hbm] * len(large),
        out_specs=tuple(vmem for _ in outs),
        scratch_shapes=list(scratch.values()),
        compiler_params=pltpu.CompilerParams(collective_id=ident, has_side_effects=True, vmem_limit_bytes=67 * 1000 * 1000),
        cost_estimate=pl.CostEstimate(flops=flops, bytes_accessed=flops // 1500, transcendentals=0),
        name='ring_' + str(ident),
    )(*small.values(), *large.values())
    return dict(zip(outs, result))


def attn_kernel(q_ref, k_ref, v_ref, kc_ref, vc_ref, slot_ref, pos_ref, o_ref, ko_ref, vo_ref, so_ref):
    blocks, _, _, width = q_ref.shape
    toks = blocks * 8
    q = (q_ref[...].reshape(toks, width) * SCORE_SCALE).astype(BF16)
    kn = k_ref[...].reshape(toks, width).astype(BF16)
    vn = v_ref[...].reshape(toks, width).astype(BF16)
    kc, vc = kc_ref[0], vc_ref[0]
    seq = pl.ds(pl.program_id(0), 1)
    slot, pos_row = slot_ref[seq, :], pos_ref[seq, :]
    pos_mat = jnp.broadcast_to(pos_row, (toks, toks))
    pos_mat_t = pos_mat.T
    pos_col = pos_mat_t[:, :1]
    row_i = lax.broadcasted_iota(jnp.int32, (toks, toks), 0)
    col_i = lax.broadcasted_iota(jnp.int32, (toks, toks), 1)
    doc_col = jnp.sum(jnp.where((pos_mat == 0) & (col_i <= row_i), 1.0, 0.0), axis=1, keepdims=True)
    doc_row = jnp.sum(jnp.where((pos_mat_t == 0) & (row_i <= col_i), 1.0, 0.0), axis=0, keepdims=True)
    contract = (((1,), (1,)), ((), ()))
    diff_old = jnp.where(doc_col == 0, pos_col, -(2 ** 30)) - jnp.where(slot >= 0, slot, -(2 ** 29))
    keep_old = (diff_old >= 0) & (diff_old < WINDOW)
    diff_new = pos_col - pos_row
    keep_new = (diff_new >= 0) & (diff_new < WINDOW) & (doc_col == doc_row)
    s_old = jnp.where(keep_old, lax.dot_general(q, kc, contract, preferred_element_type=F32), NEG_BIG)
    s_new = jnp.where(keep_new, lax.dot_general(q, kn, contract, preferred_element_type=F32), NEG_BIG)
    top = jnp.maximum(jnp.max(s_old, axis=-1, keepdims=True), jnp.max(s_new, axis=-1, keepdims=True))
    e_old = jnp.exp(s_old - top)
    e_new = jnp.exp(s_new - top)
    denom = jnp.sum(e_old, axis=-1, keepdims=True) + jnp.sum(e_new, axis=-1, keepdims=True)
    inv = 1.0 / denom
    out = jnp.dot((e_old * inv).astype(BF16), vc, preferred_element_type=F32) + jnp.dot((e_new * inv).astype(BF16), vn, preferred_element_type=F32)
    o_ref[...] = out.astype(BF16).astype(F32).reshape(o_ref.shape)
    window = kc.shape[0]
    target_row = lax.rem(pos_row, window)
    target_col = lax.rem(pos_col, window)
    hit = lax.broadcasted_iota(jnp.int32, (window, toks), 0) == target_row
    pick = jnp.where(hit, 1.0, 0.0)
    any_hit = jnp.max(pick, axis=1, keepdims=True) > 0.0
    pick = pick.astype(BF16)
    ko_ref[0] = jnp.where(any_hit, jnp.dot(pick, kn, preferred_element_type=F32), kc.astype(F32)).astype(BF16)
    vo_ref[0] = jnp.where(any_hit, jnp.dot(pick, vn, preferred_element_type=F32), vc.astype(F32)).astype(BF16)
    hit_t = lax.broadcasted_iota(jnp.int32, (toks, window), 1) == target_col
    newest = jnp.max(jnp.where(hit_t, pos_col, -1), axis=0, keepdims=True)
    so_ref[seq, :] = jnp.where(newest >= 0, newest, slot)


def attn_call(q, k, v, k_cache, v_cache, slot_pos, seg_pos):
    seqs, toks = seg_pos.shape
    width = q.shape[-1]
    blocks = toks // 8
    window = k_cache.shape[1]
    shape4 = (blocks, seqs, 8, width)
    tok_spec = pl.BlockSpec((blocks, 1, 8, width), lambda s: (0, s, 0, 0))
    cache_spec = pl.BlockSpec((1, window, width), lambda s: (s, 0, 0))
    row_spec = lambda n: pl.BlockSpec((seqs, n), lambda s: (0, 0))
    out, k_out, v_out, slot_out = pl.pallas_call(
        attn_kernel,
        grid=(seqs,),
        out_shape=(jax.ShapeDtypeStruct(shape4, F32), jax.ShapeDtypeStruct(k_cache.shape, BF16), jax.ShapeDtypeStruct(v_cache.shape, BF16), jax.ShapeDtypeStruct((seqs, window), jnp.int32)),
        in_specs=[tok_spec, tok_spec, tok_spec, cache_spec, cache_spec, row_spec(window), row_spec(toks)],
        out_specs=(tok_spec, cache_spec, cache_spec, row_spec(window)),
        cost_estimate=pl.CostEstimate(flops=8 * seqs * toks * window * width, bytes_accessed=8 * seqs * window * width, transcendentals=0),
        name='attention',
    )(q, k, v, k_cache, v_cache, slot_pos, seg_pos)
    return out, k_out, v_out, slot_out


def solution(mesh):
    tp = mesh.shape['tp']

    def device_body(x_in, seg_pos, conv_state, lru_state, k_cache, v_cache, slot_pos, norm_scale, w_x, b_x, w_y, b_y, conv_w, conv_b, w_a, b_a, w_i, b_i, a_param, w_out, b_out, w_q, w_k, w_v, w_o, b_o, w_1, b_1, w_2, b_2, w_d, b_d):
        seqs, toks = seg_pos.shape
        dim = x_in.shape[-1]
        x = x_in.reshape(-1, dim)
        soft = jax.nn.softplus(a_param)
        half = ROPE_DIM // 2
        timescale = 10000.0 ** (2.0 * jnp.arange(half).astype(F32) / ROPE_DIM)
        order = seg_pos.reshape(seqs, toks // 8, 8).swapaxes(0, 1).reshape(-1)
        angle = order[:, None].astype(F32) / timescale
        sin, cos = jnp.sin(angle), jnp.cos(angle)
        cos2 = jnp.concatenate([cos, cos], axis=1)
        sin2 = jnp.concatenate([-sin, sin], axis=1)

        width = w_q.shape[-1]
        shape4 = (tp, seqs, 8, width)
        tall = jax.ShapeDtypeStruct(shape4, F32)
        inside = (lax.broadcasted_iota(jnp.int32, (3, 8, width), 1) >= jnp.array((1, 2, 4), jnp.int32)[:, None, None]).astype(F32)

        def mlp_step(m):
            return dict(kind='mlp', idx=m, loads=(('w_1s', 'w_1', m), ('w_2s', 'w_2', m), ('w_ds', 'w_d', m)))

        def rec_step(layer):
            return dict(kind='rec', idx=layer, loads=(('p_0', 'w_x', layer), ('p_1', 'w_y', layer)))

        def out_step(layer):
            return dict(kind='pre', idx=layer, loads=(('w_pre', 'w_out', layer),))
        mlp_small = dict(norm=norm_scale, b_1=b_1, b_2=b_2, b_d=b_d)
        mlp_large = dict(w_1=w_1, w_2=w_2, w_d=w_d)
        rec_small = dict(mlp_small, b_pre=b_out, b_x=b_x, b_y=b_y, reset=(seg_pos == 0).astype(F32)[:, :, None], inside=inside, conv_state=conv_state,
                         lru_state=lru_state, conv_w=conv_w, conv_b=conv_b, w_a=w_a, b_a=b_a, w_i=w_i, b_i=b_i, soft=soft)
        rec_large = dict(mlp_large, w_x=w_x, w_y=w_y, w_out=w_out)
        rec_outs = dict(o_conv=jax.ShapeDtypeStruct(conv_state.shape[1:], BF16), o_lru=jax.ShapeDtypeStruct(lru_state.shape[1:], F32))
        work = dict(u=pltpu.VMEM(shape4, F32), y=pltpu.VMEM(shape4, F32), pad=pltpu.VMEM((toks + 8, width), F32))
        zero = comm_call(tp, 0, x, (rec_step(0), out_step(0), mlp_step(0)), rec_small, rec_large, rec_outs, work)
        one = comm_call(
            tp, 1, zero['o_x'],
            (rec_step(1), out_step(1), mlp_step(1), dict(kind='attn', idx=0, loads=(('p_0', 'w_q', None), ('p_1', 'w_k', None), ('p_2', 'w_v', None)))),
            dict(rec_small, cos=cos2, sin=sin2), dict(rec_large, w_q=w_q, w_k=w_k, w_v=w_v), dict(rec_outs, o_q=tall, o_k=tall, o_v=tall), work)
        mid, k_out, v_out, slot_out = attn_call(one['o_q'], one['o_k'], one['o_v'], k_cache, v_cache, slot_pos, seg_pos)
        last = comm_call(
            tp, 2, one['o_x'], (dict(kind='pre', idx=0, loads=(('w_pre', 'w_o', None),)), mlp_step(2)),
            dict(mlp_small, b_pre=b_o[None, :], mid=mid), dict(mlp_large, w_o=w_o), {}, {})
        conv_out = jnp.stack([zero['o_conv'], one['o_conv']])
        lru_out = jnp.stack([zero['o_lru'], one['o_lru']])
        return last['o_x'].reshape(x_in.shape), conv_out, lru_out, k_out, v_out, slot_out

    col_spec = P(None, None, 'tp')
    vec_spec = P(None, 'tp')
    block_spec = P(None, 'tp', None, None)
    row_spec = P(None, 'tp', None)
    cache_spec = P('dp', None, None)
    arg_specs = (P('dp', 'tp', None), P('dp', None), P(None, 'dp', None, 'tp'), P(None, 'dp', 'tp'), cache_spec, cache_spec, P('dp', None), P(), col_spec, vec_spec, col_spec, vec_spec, col_spec, vec_spec, block_spec, vec_spec, block_spec, vec_spec, vec_spec, row_spec, P(), P(None, 'tp'), P(), P(), P('tp', None), P(), col_spec, vec_spec, col_spec, vec_spec, row_spec, P())
    result_specs = (P('dp', 'tp', None), P(None, 'dp', None, 'tp'), P(None, 'dp', 'tp'), cache_spec, cache_spec, P('dp', None))
    return jax.shard_map(device_body, mesh=mesh, in_specs=arg_specs, out_specs=result_specs, check_vma=False)
```

```python
import functools

import jax
import jax.numpy as jnp
from jax import lax
from jax.experimental import pallas as pl
from jax.experimental.pallas import tpu as pltpu
from jax.sharding import PartitionSpec as P

WINDOW = 2048
HEAD_DIM = 256
ROPE_DIM = 128
CONV_WIDTH = 4
SCORE_SCALE = 0.0625
NEG_BIG = -1e30
F32 = jnp.float32
BF16 = jnp.bfloat16

SLOT_REL = (0, -1, 1, -2, 2, -3, 3, 4)
ROW_TILE = 16


def slot_of(rel):
    if rel == 0:
        return 0
    if rel in (4, -4):
        return 7
    return -2 * rel - 1 if rel < 0 else 2 * rel


class Net:
    def __init__(self, tp, rows, dim, r):
        self.me = lax.axis_index('tp')
        self.core = lax.rem(self.me, 2)
        self.chips = tp // 2
        self.chip = lax.div(self.me, 2)
        self.up = lax.rem(self.me + 2, tp)
        self.down = lax.rem(self.me + tp - 2, tp)
        self.partner = self.me + 1 - 2 * self.core
        self.rows = rows
        self.groups = rows // ROW_TILE
        self.dim = dim
        self.cw = dim // 2
        self.r = r

    def barrier(self):
        sem = pltpu.get_barrier_semaphore()
        for other in (self.up, self.down, self.partner):
            pl.semaphore_signal(sem, inc=1, device_id={'tp': other}, device_id_type=pl.DeviceIdType.MESH)
        pl.semaphore_wait(sem, 3)

    def span(self, chunk):
        half, group = chunk
        cols, rows = half * self.cw, group * ROW_TILE
        if not isinstance(half, int):
            cols = pl.multiple_of(cols, 128)
        if not isinstance(group, int):
            rows = pl.multiple_of(rows, ROW_TILE)
        return pl.ds(rows, ROW_TILE), pl.ds(cols, self.cw)

    def remote(self, src, dst, send, recv, dev):
        return pltpu.make_async_remote_copy(src_ref=src, dst_ref=dst, send_sem=send, recv_sem=recv, device_id={'tp': dev}, device_id_type=pl.DeviceIdType.MESH)

    def ag_hop(self, way, d, chunk):
        sign = -1 if way == 0 else 1
        src, dst = slot_of(sign * (d - 1)), slot_of(sign * d)
        g, sems = self.r['g'], (way, d - 1) + chunk
        return self.remote(g.at[(2 * src + self.core,) + self.span(chunk)], g.at[(2 * dst + self.core,) + self.span(chunk)],
                           self.r['send_z'].at[sems], self.r['ag_z'].at[sems], self.up if way == 0 else self.down)

    def ag_pair(self, slot, chunk):
        ref, sems = self.r['g'].at[(2 * slot + self.core,) + self.span(chunk)], (slot,) + chunk
        return self.remote(ref, ref, self.r['send_d'].at[sems], self.r['ag_d'].at[sems], self.partner)

    def rs_pair(self, slot, chunk):
        idx, sems = (slot,) + self.span(chunk), (slot,) + chunk
        return self.remote(self.r['dsend'].at[idx], self.r['drecv'].at[idx], self.r['give_d'].at[sems], self.r['rs_d'].at[sems], self.partner)

    def rs_hop(self, way, d, chunk):
        idx, sems = (way, d - 1) + self.span(chunk), (way, d - 1) + chunk
        return self.remote(self.r['zsend'].at[idx], self.r['zrecv'].at[idx], self.r['give_z'].at[sems], self.r['rs_z'].at[sems], self.up if way == 0 else self.down)

    def chunks(self):
        return [(half, group) for group in range(self.groups) for half in range(2)]

    def hops(self):
        for way in range(2):
            for d in range(1, 5):
                for chunk in self.chunks():
                    if d < 4 or chunk[0] == way:
                        yield way, d, chunk

    def abs_chip(self, rel):
        return lax.rem(self.chip + (rel + self.chips), self.chips)

    def wait_pair(self, slots):
        for slot in slots:
            for chunk in self.chunks():
                self.ag_pair(slot, chunk).wait_recv()

    def gather_start(self, group):
        for k in range(2):
            self.ag_hop(0, 1, (k, group)).start()
            self.ag_hop(1, 1, (1 - k, group)).start()
        for k in range(2):
            self.ag_pair(0, (k, group)).start()

    def gather(self, run_pass):
        for d in range(1, 5):
            for p in range(2 * self.groups if d < 4 else self.groups):
                for way in range(2):
                    chunk = ((p + way) % 2, p // 2) if d < 4 else (way, p)
                    self.ag_hop(way, d, chunk).wait_recv()
                    if d < 3 or (d == 3 and chunk[0] == way):
                        self.ag_hop(way, d + 1, chunk).start()
                    self.ag_pair(slot_of(-d if way == 0 else d), chunk).start()
                if p == 0 and d > 1:
                    first = 0 if d == 2 else 2 * d - 3
                    self.wait_pair(range(first, 2 * d - 1))
                    run_pass(first, 2 * d - 1)

    def gather_end(self, run_pass):
        self.wait_pair((7,))
        run_pass(7, 8)
        for way, d, chunk in self.hops():
            self.ag_hop(way, d, chunk).wait_send()
        for slot in range(8):
            for chunk in self.chunks():
                self.ag_pair(slot, chunk).wait_send()

    def reduce(self, lhs_of, w_ref, finish, between=None):
        r, rows = self.r, self.rows
        sub = min(512, self.cw)
        steps = self.cw // sub

        def slots_of(d):
            return {4: (7,), 0: (0,)}.get(d, (slot_of(-d), slot_of(d)))

        def compute(d):
            slots = slots_of(d)

            def one_half(half, outer):
                def body(t, carry):
                    span = pl.ds(pl.multiple_of(half * self.cw + t * sub, sub), sub)
                    lhs = jnp.concatenate([lhs_of(s, self.core) for s in slots] + [lhs_of(s, 1 - self.core) for s in slots], axis=0)
                    out = jnp.dot(lhs, w_ref[:, span], preferred_element_type=F32)
                    for i, s in enumerate(slots):
                        j = len(slots) + i
                        r['pown'][s, :, span] = out[i * rows:(i + 1) * rows]
                        r['dsend'][s, :, span] = out[j * rows:(j + 1) * rows].astype(BF16)
                    return carry
                lax.fori_loop(0, steps, body, 0)
                for group in range(self.groups):
                    for s in slots:
                        self.rs_pair(s, (half, group)).start()
                return outer
            lax.fori_loop(0, 2, one_half, 0)

        def combine(way, d, chunk):
            s = slot_of(d if way == 0 else -d)
            idx = self.span(chunk)
            self.rs_pair(s, chunk).wait_recv()
            total = r['pown'][(s,) + idx] + r['drecv'][(s,) + idx].astype(F32)
            if d < 3 or (d == 3 and chunk[0] == way):
                self.rs_hop(way, d + 1, chunk).wait_recv()
                total = total + r['zrecv'][(way, d) + idx].astype(F32)
            r['zsend'][(way, d - 1) + idx] = total.astype(BF16)
            self.rs_hop(way, d, chunk).start()

        def send(d, deep):
            def body(group, carry):
                for way in range(2):
                    combine(way, d, (way if deep else 1 - way, group))
                return carry
            lax.fori_loop(0, self.groups, body, 0)

        compute(3)
        for way in (1, 0):
            lax.fori_loop(0, self.groups, lambda group, carry, way=way: (combine(way, 3, (1 - way, group)), carry)[1], 0)
        compute(2)
        if between is not None:
            between()
        compute(4)
        send(2, False)
        send(4, True)
        compute(1)
        send(3, True)
        send(1, False)
        compute(0)
        send(2, True)
        send(1, True)
        for group in range(self.groups):
            for half in range(2):
                self.rs_pair(0, (half, group)).wait_recv()
                self.rs_hop(0, 1, (half, group)).wait_recv()
                self.rs_hop(1, 1, (half, group)).wait_recv()
                idx = self.span((half, group))
                total = r['pown'][(0,) + idx] + r['drecv'][(0,) + idx].astype(F32)
                total = total + r['zrecv'][(0, 0) + idx].astype(F32) + r['zrecv'][(1, 0) + idx].astype(F32)
                finish(idx, total)
            yield group

    def reduce_end(self):
        for way, d, chunk in self.hops():
            self.rs_hop(way, d, chunk).wait_send()

        def body(slot, carry):
            for chunk in self.chunks():
                self.rs_pair(slot, chunk).wait_send()
            return carry
        lax.fori_loop(0, 8, body, 0)


def column_of(row):
    n = row.shape[1]
    return jnp.broadcast_to(row, (n, n)).T[:, :1]


def recurrence(layer, r):
    u_ref, y_ref, pad = r['u'], r['y'], r['pad']
    blocks, seqs, _, width = u_ref.shape
    toks = blocks * 8

    def one_seq(s, carry):
        u = u_ref[:, s].reshape(toks, width)
        pad[8:8 + toks, :] = u
        for j in range(CONV_WIDTH - 1):
            pad[5 + j:6 + j, :] = r['conv_state'][s, j].astype(F32)[layer:layer + 1]
        r['o_conv'][s] = u[toks - 3:, :].astype(BF16)
        total = jnp.zeros((toks, width), F32)
        for j in range(CONV_WIDTH):
            total = total + pad[5 + j:5 + j + toks, :] * r['conv_w'][layer, j:j + 1, :].astype(F32)
        row_of = lambda key: r[key][layer:layer + 1, :].astype(F32)
        conv = (total + row_of('conv_b')).astype(BF16)
        gate_r = jax.nn.sigmoid(jnp.dot(conv, r['w_a'][layer, 0], preferred_element_type=F32) + row_of('b_a'))
        gate_i = jax.nn.sigmoid(jnp.dot(conv, r['w_i'][layer, 0], preferred_element_type=F32) + row_of('b_i'))
        decay = jnp.exp(-8.0 * gate_r * row_of('soft'))
        reset = column_of(r['seg_pos'][pl.ds(s, 1), :]) == 0
        mult = jnp.where(reset, 1.0, jnp.sqrt(1.0 - decay * decay))
        decay = jnp.where(reset, 0.0, decay)
        drive = conv.astype(F32) * gate_i * mult
        a = decay.reshape(blocks, 8, width)
        b = drive.reshape(blocks, 8, width)
        row = lax.broadcasted_iota(jnp.int32, (blocks, 8, width), 1)
        for k in (1, 2, 4):
            inside = row >= k
            a_sh = jnp.where(inside, pltpu.roll(a, k, 1), 1.0)
            b_sh = jnp.where(inside, pltpu.roll(b, k, 1), 0.0)
            b = a * b_sh + b
            a = a * a_sh
        state = r['lru_state'][s, layer:layer + 1, :]
        for blk in range(blocks):
            h = a[blk] * state + b[blk]
            state = h[7:8, :]
            u_ref[blk, s] = h * y_ref[blk, s]
        r['o_lru'][pl.ds(s, 1), :] = state
        return carry
    lax.fori_loop(0, seqs, one_seq, 0)


def comm_kernel(plan, tp, names, outs, scratch, *refs):
    r = dict(zip(names + outs + scratch, refs))
    x_ref = r['x']
    rows, dim = x_ref.shape
    net = Net(tp, rows, dim, r)
    loads = [[] for _ in plan]
    count = 0
    for i, step in enumerate(plan):
        for key, src, layer in step['loads']:
            view = r[src] if layer is None else r[src].at[layer]
            loads[i].append((key, pltpu.make_async_copy(view, r[key], r['w_sem'].at[count])))
            count += 1
    used = set()
    for step in loads:
        for key, copy in step:
            if key not in used:
                used.add(key)
                copy.start()

    def refill(i):
        for key, _ in loads[i]:
            later = [copy for step in loads[i + 1:] for k, copy in step if k == key]
            if later:
                later[0].start()

    net.barrier()
    xbuf = r['xbuf']
    xbuf[...] = x_ref[...]
    groups = range(net.groups)

    def enter(idx, steps):
        for group in groups if steps is None else steps:
            span = pl.ds(group * ROW_TILE, ROW_TILE)
            h = xbuf[span, :].astype(F32)
            inv = lax.rsqrt(jnp.mean(h * h, axis=-1, keepdims=True) + 1e-6)
            r['g'][net.core, span, :] = (h * inv * (1.0 + r['norm'][idx:idx + 1, :].astype(F32))).astype(BF16)
            net.gather_start(group)
        if steps is not None:
            net.reduce_end()

    def finish_with(bias_ref, idx):
        def finish(span, total):
            xbuf[span] = (xbuf[span].astype(F32) + total + bias_ref[idx:idx + 1, span[1]].astype(F32)).astype(BF16)
        return finish

    def block_of(first, last):
        return r['g'][2 * first:2 * last].reshape((last - first) * 2 * rows, dim)

    def wait_loads(i):
        pending = list(loads[i])

        def wait():
            while pending:
                pending.pop()[1].wait()
        return wait

    reduction = None
    for i, step in enumerate(plan):
        kind, idx = step['kind'], step['idx']
        ready = wait_loads(i)
        if kind == 'pre':
            ready()
            source = r['mid'] if 'mid' in r else r['u']
            r['apre'][...] = source[...].reshape(r['apre'].shape).astype(BF16)

            def lhs_pre(slot, core):
                blk = 2 * net.abs_chip(SLOT_REL[slot]) + core
                return r['apre'][pl.ds(pl.multiple_of(blk * rows, 16), rows), :]
            reduction = net.reduce(lhs_pre, r['w_pre'], finish_with(r['b_pre'], idx))
            owner = i
        elif kind == 'mlp':
            def mlp_pass(first, last, ready=ready, m=idx):
                ready()
                width = 2 * (last - first)

                def body(t, carry):
                    cols = pl.ds(pl.multiple_of(t * 256, 256), 256)
                    lhs = block_of(first, last)
                    h1 = jnp.dot(lhs, r['w_1s'][:, cols], preferred_element_type=F32) + r['b_1'][m:m + 1, cols].astype(F32)
                    h2 = jnp.dot(lhs, r['w_2s'][:, cols], preferred_element_type=F32) + r['b_2'][m:m + 1, cols].astype(F32)
                    act = (jax.nn.gelu(h1, approximate=True) * h2).astype(BF16)
                    r['act'][2 * first:2 * last, :, cols] = act.reshape(width, rows, 256)
                    return carry
                lax.fori_loop(0, r['w_1s'].shape[1] // 256, body, 0)
            enter(2 * idx + 1, reduction)
            refill(owner)
            net.gather(mlp_pass)
            reduction = net.reduce(lambda slot, core: r['act'][2 * slot + core], r['w_ds'], finish_with(r['b_d'], idx), functools.partial(net.gather_end, mlp_pass))
            owner = i
        else:
            def post_pass(first, last, ready=ready, kind=kind, layer=idx):
                ready()
                lhs = block_of(first, last)
                chips = [net.abs_chip(SLOT_REL[s]) for s in range(first, last)]

                def put(ref, value, rope=False):
                    for n, chip in enumerate(chips):
                        v = value[n * 2 * rows:(n + 1) * 2 * rows]
                        if rope:
                            span = pl.ds(pl.multiple_of(chip * 2 * rows, 16), 2 * rows)
                            lo = v[:, :ROPE_DIM]
                            lo = lo * r['cos'][span, :] + pltpu.roll(lo, ROPE_DIM // 2, 1) * r['sin'][span, :]
                            v = jnp.concatenate([lo, v[:, ROPE_DIM:]], axis=1)
                        ref[pl.ds(2 * chip, 2)] = v.astype(BF16).astype(F32).reshape((2,) + ref.shape[1:])
                if kind == 'rec':
                    put(r['u'], jnp.dot(lhs, r['p_0'][...], preferred_element_type=F32) + r['b_x'][layer:layer + 1, :].astype(F32))
                    put(r['y'], jax.nn.gelu(jnp.dot(lhs, r['p_1'][...], preferred_element_type=F32) + r['b_y'][layer:layer + 1, :].astype(F32), approximate=True))
                else:
                    put(r['o_q'], jnp.dot(lhs, r['p_0'][...], preferred_element_type=F32), True)
                    put(r['o_k'], jnp.dot(lhs, r['p_1'][...], preferred_element_type=F32), True)
                    put(r['o_v'], jnp.dot(lhs, r['p_2'][...], preferred_element_type=F32))
            enter(4 if kind == 'attn' else 2 * idx, reduction)
            if reduction is not None:
                refill(owner)
            net.gather(post_pass)
            net.gather_end(post_pass)
            refill(i)
            reduction = None
            if kind == 'rec':
                recurrence(idx, r)
    if reduction is not None:
        for _ in reduction:
            pass
        net.reduce_end()
    r['o_x'][...] = xbuf[...]


def comm_call(tp, ident, x, plan, small, large, outs, extra):
    rows, dim = x.shape
    vmem, hbm = pl.BlockSpec(memory_space=pltpu.VMEM), pl.BlockSpec(memory_space=pl.ANY)
    small = dict(x=x, **small)
    names = list(small) + list(large)
    outs = dict(o_x=jax.ShapeDtypeStruct((rows, dim), BF16), **outs)
    scratch = dict(extra)
    flops = 0
    total = 0
    for step in plan:
        for key, src, layer in step['loads']:
            shape = large[src].shape[-2:]
            scratch.setdefault(key, pltpu.VMEM(shape, BF16))
            flops += 2 * tp * rows * shape[0] * shape[1]
            total += 1
    scratch['pown'] = pltpu.VMEM((8, rows, dim), F32)
    scratch['dsend'] = pltpu.VMEM((8, rows, dim), BF16)
    scratch['drecv'] = pltpu.VMEM((8, rows, dim), BF16)
    scratch['zsend'] = pltpu.VMEM((2, 4, rows, dim), BF16)
    scratch['zrecv'] = pltpu.VMEM((2, 4, rows, dim), BF16)
    scratch['act'] = pltpu.VMEM((tp, rows, scratch['w_1s'].shape[1]), BF16)
    scratch['apre'] = pltpu.VMEM((tp * rows, scratch['w_pre'].shape[0]), BF16)
    scratch['g'] = pltpu.VMEM((tp, rows, dim), BF16)
    scratch['xbuf'] = pltpu.VMEM((rows, dim), BF16)
    for key in ('ag_z', 'rs_z', 'send_z', 'give_z'):
        scratch[key] = pltpu.SemaphoreType.DMA((2, 4, 2, rows // ROW_TILE))
    for key in ('ag_d', 'rs_d', 'send_d', 'give_d'):
        scratch[key] = pltpu.SemaphoreType.DMA((8, 2, rows // ROW_TILE))
    scratch['w_sem'] = pltpu.SemaphoreType.DMA((total,))
    result = pl.pallas_call(
        functools.partial(comm_kernel, plan, tp, names, list(outs), list(scratch)),
        out_shape=tuple(outs.values()),
        in_specs=[vmem] * len(small) + [hbm] * len(large),
        out_specs=tuple(vmem for _ in outs),
        scratch_shapes=list(scratch.values()),
        compiler_params=pltpu.CompilerParams(collective_id=ident, has_side_effects=True, vmem_limit_bytes=67 * 1000 * 1000),
        cost_estimate=pl.CostEstimate(flops=flops, bytes_accessed=flops // 1500, transcendentals=0),
        name='ring_' + str(ident),
    )(*small.values(), *large.values())
    return dict(zip(outs, result))


def attn_kernel(q_ref, k_ref, v_ref, kc_ref, vc_ref, slot_ref, pos_ref, o_ref, ko_ref, vo_ref, so_ref):
    blocks, _, _, width = q_ref.shape
    toks = blocks * 8
    q = (q_ref[...].reshape(toks, width) * SCORE_SCALE).astype(BF16)
    kn = k_ref[...].reshape(toks, width).astype(BF16)
    vn = v_ref[...].reshape(toks, width).astype(BF16)
    kc, vc = kc_ref[0], vc_ref[0]
    seq = pl.ds(pl.program_id(0), 1)
    slot, pos_row = slot_ref[seq, :], pos_ref[seq, :]
    pos_mat = jnp.broadcast_to(pos_row, (toks, toks))
    pos_mat_t = pos_mat.T
    pos_col = pos_mat_t[:, :1]
    row_i = lax.broadcasted_iota(jnp.int32, (toks, toks), 0)
    col_i = lax.broadcasted_iota(jnp.int32, (toks, toks), 1)
    doc_col = jnp.sum(jnp.where((pos_mat == 0) & (col_i <= row_i), 1.0, 0.0), axis=1, keepdims=True)
    doc_row = jnp.sum(jnp.where((pos_mat_t == 0) & (row_i <= col_i), 1.0, 0.0), axis=0, keepdims=True)
    contract = (((1,), (1,)), ((), ()))
    diff_old = jnp.where(doc_col == 0, pos_col, -(2 ** 30)) - jnp.where(slot >= 0, slot, -(2 ** 29))
    keep_old = (diff_old >= 0) & (diff_old < WINDOW)
    diff_new = pos_col - pos_row
    keep_new = (diff_new >= 0) & (diff_new < WINDOW) & (doc_col == doc_row)
    s_old = jnp.where(keep_old, lax.dot_general(q, kc, contract, preferred_element_type=F32), NEG_BIG)
    s_new = jnp.where(keep_new, lax.dot_general(q, kn, contract, preferred_element_type=F32), NEG_BIG)
    top = jnp.maximum(jnp.max(s_old, axis=-1, keepdims=True), jnp.max(s_new, axis=-1, keepdims=True))
    e_old = jnp.exp(s_old - top)
    e_new = jnp.exp(s_new - top)
    denom = jnp.sum(e_old, axis=-1, keepdims=True) + jnp.sum(e_new, axis=-1, keepdims=True)
    inv = 1.0 / denom
    out = jnp.dot((e_old * inv).astype(BF16), vc, preferred_element_type=F32) + jnp.dot((e_new * inv).astype(BF16), vn, preferred_element_type=F32)
    o_ref[...] = out.astype(BF16).astype(F32).reshape(o_ref.shape)
    window = kc.shape[0]
    target_row = lax.rem(pos_row, window)
    target_col = lax.rem(pos_col, window)
    hit = lax.broadcasted_iota(jnp.int32, (window, toks), 0) == target_row
    pick = jnp.where(hit, 1.0, 0.0)
    any_hit = jnp.max(pick, axis=1, keepdims=True) > 0.0
    pick = pick.astype(BF16)
    ko_ref[0] = jnp.where(any_hit, jnp.dot(pick, kn, preferred_element_type=F32), kc.astype(F32)).astype(BF16)
    vo_ref[0] = jnp.where(any_hit, jnp.dot(pick, vn, preferred_element_type=F32), vc.astype(F32)).astype(BF16)
    hit_t = lax.broadcasted_iota(jnp.int32, (toks, window), 1) == target_col
    newest = jnp.max(jnp.where(hit_t, pos_col, -1), axis=0, keepdims=True)
    so_ref[seq, :] = jnp.where(newest >= 0, newest, slot)


def attn_call(q, k, v, k_cache, v_cache, slot_pos, seg_pos):
    seqs, toks = seg_pos.shape
    width = q.shape[-1]
    blocks = toks // 8
    window = k_cache.shape[1]
    shape4 = (blocks, seqs, 8, width)
    tok_spec = pl.BlockSpec((blocks, 1, 8, width), lambda s: (0, s, 0, 0))
    cache_spec = pl.BlockSpec((1, window, width), lambda s: (s, 0, 0))
    row_spec = lambda n: pl.BlockSpec((seqs, n), lambda s: (0, 0))
    out, k_out, v_out, slot_out = pl.pallas_call(
        attn_kernel,
        grid=(seqs,),
        out_shape=(jax.ShapeDtypeStruct(shape4, F32), jax.ShapeDtypeStruct(k_cache.shape, BF16), jax.ShapeDtypeStruct(v_cache.shape, BF16), jax.ShapeDtypeStruct((seqs, window), jnp.int32)),
        in_specs=[tok_spec, tok_spec, tok_spec, cache_spec, cache_spec, row_spec(window), row_spec(toks)],
        out_specs=(tok_spec, cache_spec, cache_spec, row_spec(window)),
        cost_estimate=pl.CostEstimate(flops=8 * seqs * toks * window * width, bytes_accessed=8 * seqs * window * width, transcendentals=0),
        name='attention',
    )(q, k, v, k_cache, v_cache, slot_pos, seg_pos)
    return out, k_out, v_out, slot_out


def solution(mesh):
    tp = mesh.shape['tp']

    def device_body(x_in, seg_pos, conv_state, lru_state, k_cache, v_cache, slot_pos, norm_scale, w_x, b_x, w_y, b_y, conv_w, conv_b, w_a, b_a, w_i, b_i, a_param, w_out, b_out, w_q, w_k, w_v, w_o, b_o, w_1, b_1, w_2, b_2, w_d, b_d):
        seqs, toks = seg_pos.shape
        dim = x_in.shape[-1]
        x = x_in.reshape(-1, dim)
        soft = jax.nn.softplus(a_param)
        half = ROPE_DIM // 2
        timescale = 10000.0 ** (2.0 * jnp.arange(half).astype(F32) / ROPE_DIM)
        order = seg_pos.reshape(seqs, toks // 8, 8).swapaxes(0, 1).reshape(-1)
        angle = order[:, None].astype(F32) / timescale
        sin, cos = jnp.sin(angle), jnp.cos(angle)
        cos2 = jnp.concatenate([cos, cos], axis=1)
        sin2 = jnp.concatenate([-sin, sin], axis=1)

        width = w_q.shape[-1]
        shape4 = (tp, seqs, 8, width)
        tall = jax.ShapeDtypeStruct(shape4, F32)

        def mlp_step(m):
            return dict(kind='mlp', idx=m, loads=(('w_1s', 'w_1', m), ('w_2s', 'w_2', m), ('w_ds', 'w_d', m)))

        def rec_step(layer):
            return dict(kind='rec', idx=layer, loads=(('p_0', 'w_x', layer), ('p_1', 'w_y', layer)))

        def out_step(layer):
            return dict(kind='pre', idx=layer, loads=(('w_pre', 'w_out', layer),))
        mlp_small = dict(norm=norm_scale, b_1=b_1, b_2=b_2, b_d=b_d)
        mlp_large = dict(w_1=w_1, w_2=w_2, w_d=w_d)
        rec_small = dict(mlp_small, b_pre=b_out, b_x=b_x, b_y=b_y, seg_pos=seg_pos, conv_state=conv_state.transpose(1, 2, 0, 3),
                         lru_state=lru_state.swapaxes(0, 1), conv_w=conv_w, conv_b=conv_b, w_a=w_a, b_a=b_a, w_i=w_i, b_i=b_i, soft=soft)
        rec_large = dict(mlp_large, w_x=w_x, w_y=w_y, w_out=w_out)
        rec_outs = dict(o_conv=jax.ShapeDtypeStruct(conv_state.shape[1:], BF16), o_lru=jax.ShapeDtypeStruct(lru_state.shape[1:], F32))
        work = dict(u=pltpu.VMEM(shape4, F32), y=pltpu.VMEM(shape4, F32), pad=pltpu.VMEM((toks + 8, width), F32))
        zero = comm_call(tp, 0, x, (rec_step(0), out_step(0), mlp_step(0)), rec_small, rec_large, rec_outs, work)
        one = comm_call(
            tp, 1, zero['o_x'],
            (rec_step(1), out_step(1), mlp_step(1), dict(kind='attn', idx=0, loads=(('p_0', 'w_q', None), ('p_1', 'w_k', None), ('p_2', 'w_v', None)))),
            dict(rec_small, cos=cos2, sin=sin2), dict(rec_large, w_q=w_q, w_k=w_k, w_v=w_v), dict(rec_outs, o_q=tall, o_k=tall, o_v=tall), work)
        mid, k_out, v_out, slot_out = attn_call(one['o_q'], one['o_k'], one['o_v'], k_cache, v_cache, slot_pos, seg_pos)
        last = comm_call(
            tp, 2, one['o_x'], (dict(kind='pre', idx=0, loads=(('w_pre', 'w_o', None),)), mlp_step(2)),
            dict(mlp_small, b_pre=b_o[None, :], mid=mid), dict(mlp_large, w_o=w_o), {}, {})
        conv_out = jnp.stack([zero['o_conv'], one['o_conv']], axis=2).transpose(2, 0, 1, 3)
        lru_out = jnp.stack([zero['o_lru'], one['o_lru']], axis=1).swapaxes(0, 1)
        return last['o_x'].reshape(x_in.shape), conv_out, lru_out, k_out, v_out, slot_out

    col_spec = P(None, None, 'tp')
    vec_spec = P(None, 'tp')
    block_spec = P(None, 'tp', None, None)
    row_spec = P(None, 'tp', None)
    cache_spec = P('dp', None, None)
    arg_specs = (P('dp', 'tp', None), P('dp', None), P(None, 'dp', None, 'tp'), P(None, 'dp', 'tp'), cache_spec, cache_spec, P('dp', None), P(), col_spec, vec_spec, col_spec, vec_spec, col_spec, vec_spec, block_spec, vec_spec, block_spec, vec_spec, vec_spec, row_spec, P(), P(None, 'tp'), P(), P(), P('tp', None), P(), col_spec, vec_spec, col_spec, vec_spec, row_spec, P())
    result_specs = (P('dp', 'tp', None), P(None, 'dp', None, 'tp'), P(None, 'dp', 'tp'), cache_spec, cache_spec, P('dp', None))
    return jax.shard_map(device_body, mesh=mesh, in_specs=arg_specs, out_specs=result_specs, check_vma=False)
```

```python
import functools

import jax
import jax.numpy as jnp
from jax import lax
from jax.experimental import pallas as pl
from jax.experimental.pallas import tpu as pltpu
from jax.sharding import PartitionSpec as P

WINDOW = 2048
HEAD_DIM = 256
ROPE_DIM = 128
CONV_WIDTH = 4
SCORE_SCALE = 0.0625
NEG_BIG = -1e30
F32 = jnp.float32
BF16 = jnp.bfloat16

SLOT_REL = (0, -1, 1, -2, 2, -3, 3, 4)
ROW_TILE = 16


def slot_of(rel):
    if rel == 0:
        return 0
    if rel in (4, -4):
        return 7
    return -2 * rel - 1 if rel < 0 else 2 * rel


class Net:
    def __init__(self, tp, rows, dim, r):
        self.me = lax.axis_index('tp')
        self.core = lax.rem(self.me, 2)
        self.chips = tp // 2
        self.chip = lax.div(self.me, 2)
        self.up = lax.rem(self.me + 2, tp)
        self.down = lax.rem(self.me + tp - 2, tp)
        self.partner = self.me + 1 - 2 * self.core
        self.rows = rows
        self.groups = rows // ROW_TILE
        self.dim = dim
        self.cw = dim // 2
        self.r = r

    def greet(self):
        sem = pltpu.get_barrier_semaphore()
        for other in (self.up, self.down, self.partner):
            pl.semaphore_signal(sem, inc=1, device_id={'tp': other}, device_id_type=pl.DeviceIdType.MESH)

    def meet(self):
        pl.semaphore_wait(pltpu.get_barrier_semaphore(), 3)

    def span(self, chunk):
        half, group = chunk
        cols, rows = half * self.cw, group * ROW_TILE
        if not isinstance(half, int):
            cols = pl.multiple_of(cols, 128)
        if not isinstance(group, int):
            rows = pl.multiple_of(rows, ROW_TILE)
        return pl.ds(rows, ROW_TILE), pl.ds(cols, self.cw)

    def remote(self, src, dst, send, recv, dev):
        return pltpu.make_async_remote_copy(src_ref=src, dst_ref=dst, send_sem=send, recv_sem=recv, device_id={'tp': dev}, device_id_type=pl.DeviceIdType.MESH)

    def ag_hop(self, way, d, chunk):
        sign = -1 if way == 0 else 1
        src, dst = slot_of(sign * (d - 1)), slot_of(sign * d)
        g, sems = self.r['g'], (way, d - 1) + chunk
        return self.remote(g.at[(2 * src + self.core,) + self.span(chunk)], g.at[(2 * dst + self.core,) + self.span(chunk)],
                           self.r['send_z'].at[sems], self.r['ag_z'].at[sems], self.up if way == 0 else self.down)

    def ag_pair(self, slot, chunk):
        ref, sems = self.r['g'].at[(2 * slot + self.core,) + self.span(chunk)], (slot,) + chunk
        return self.remote(ref, ref, self.r['send_d'].at[sems], self.r['ag_d'].at[sems], self.partner)

    def rs_pair(self, slot, chunk):
        idx, sems = (slot,) + self.span(chunk), (slot,) + chunk
        return self.remote(self.r['dsend'].at[idx], self.r['drecv'].at[idx], self.r['give_d'].at[sems], self.r['rs_d'].at[sems], self.partner)

    def rs_hop(self, way, d, chunk):
        idx, sems = (way, d - 1) + self.span(chunk), (way, d - 1) + chunk
        return self.remote(self.r['zsend'].at[idx], self.r['zrecv'].at[idx], self.r['give_z'].at[sems], self.r['rs_z'].at[sems], self.up if way == 0 else self.down)

    def chunks(self):
        return [(half, group) for group in range(self.groups) for half in range(2)]

    def hops(self):
        for way in range(2):
            for d in range(1, 5):
                for chunk in self.chunks():
                    if d < 4 or chunk[0] == way:
                        yield way, d, chunk

    def abs_chip(self, rel):
        return lax.rem(self.chip + (rel + self.chips), self.chips)

    def wait_pair(self, slots):
        for slot in slots:
            for chunk in self.chunks():
                self.ag_pair(slot, chunk).wait_recv()

    def gather_start(self, group):
        for k in range(2):
            self.ag_hop(0, 1, (k, group)).start()
            self.ag_hop(1, 1, (1 - k, group)).start()
        for k in range(2):
            self.ag_pair(0, (k, group)).start()

    def gather(self, run_pass):
        for d in range(1, 5):
            for p in range(2 * self.groups if d < 4 else self.groups):
                for way in range(2):
                    chunk = ((p + way) % 2, p // 2) if d < 4 else (way, p)
                    self.ag_hop(way, d, chunk).wait_recv()
                    if d < 3 or (d == 3 and chunk[0] == way):
                        self.ag_hop(way, d + 1, chunk).start()
                    self.ag_pair(slot_of(-d if way == 0 else d), chunk).start()
                if p == 0 and d > 1:
                    first = 0 if d == 2 else 2 * d - 3
                    self.wait_pair(range(first, 2 * d - 1))
                    run_pass(first, 2 * d - 1)

    def gather_end(self, run_pass):
        self.wait_pair((7,))
        run_pass(7, 8)
        for way, d, chunk in self.hops():
            self.ag_hop(way, d, chunk).wait_send()
        for slot in range(8):
            for chunk in self.chunks():
                self.ag_pair(slot, chunk).wait_send()

    def reduce(self, lhs_of, w_ref, finish, between=None):
        r, rows = self.r, self.rows
        sub = min(512, self.cw)
        steps = self.cw // sub

        def slots_of(d):
            return {4: (7,), 0: (0,)}.get(d, (slot_of(-d), slot_of(d)))

        def compute(d):
            slots = slots_of(d)

            def one_half(half, outer):
                def body(t, carry):
                    span = pl.ds(pl.multiple_of(half * self.cw + t * sub, sub), sub)
                    lhs = jnp.concatenate([lhs_of(s, self.core) for s in slots] + [lhs_of(s, 1 - self.core) for s in slots], axis=0)
                    out = jnp.dot(lhs, w_ref[:, span], preferred_element_type=F32)
                    for i, s in enumerate(slots):
                        j = len(slots) + i
                        r['pown'][s, :, span] = out[i * rows:(i + 1) * rows]
                        r['dsend'][s, :, span] = out[j * rows:(j + 1) * rows].astype(BF16)
                    return carry
                lax.fori_loop(0, steps, body, 0)
                for group in range(self.groups):
                    for s in slots:
                        self.rs_pair(s, (half, group)).start()
                return outer
            lax.fori_loop(0, 2, one_half, 0)

        def combine(way, d, chunk):
            s = slot_of(d if way == 0 else -d)
            idx = self.span(chunk)
            self.rs_pair(s, chunk).wait_recv()
            total = r['pown'][(s,) + idx] + r['drecv'][(s,) + idx].astype(F32)
            if d < 3 or (d == 3 and chunk[0] == way):
                self.rs_hop(way, d + 1, chunk).wait_recv()
                total = total + r['zrecv'][(way, d) + idx].astype(F32)
            r['zsend'][(way, d - 1) + idx] = total.astype(BF16)
            self.rs_hop(way, d, chunk).start()

        def send(d, deep):
            def body(group, carry):
                for way in range(2):
                    combine(way, d, (way if deep else 1 - way, group))
                return carry
            lax.fori_loop(0, self.groups, body, 0)

        compute(3)
        for way in (1, 0):
            lax.fori_loop(0, self.groups, lambda group, carry, way=way: (combine(way, 3, (1 - way, group)), carry)[1], 0)
        compute(2)
        if between is not None:
            between()
        compute(4)
        send(2, False)
        send(4, True)
        compute(1)
        send(3, True)
        send(1, False)
        compute(0)
        send(2, True)
        send(1, True)
        for group in range(self.groups):
            for half in range(2):
                self.rs_pair(0, (half, group)).wait_recv()
                self.rs_hop(0, 1, (half, group)).wait_recv()
                self.rs_hop(1, 1, (half, group)).wait_recv()
                idx = self.span((half, group))
                total = r['pown'][(0,) + idx] + r['drecv'][(0,) + idx].astype(F32)
                total = total + r['zrecv'][(0, 0) + idx].astype(F32) + r['zrecv'][(1, 0) + idx].astype(F32)
                finish(idx, total)
            yield group

    def reduce_end(self):
        for way, d, chunk in self.hops():
            self.rs_hop(way, d, chunk).wait_send()

        def body(slot, carry):
            for chunk in self.chunks():
                self.rs_pair(slot, chunk).wait_send()
            return carry
        lax.fori_loop(0, 8, body, 0)


def column_of(row):
    n = row.shape[1]
    return jnp.broadcast_to(row, (n, n)).T[:, :1]


def recurrence(layer, r):
    u_ref, y_ref, pad = r['u'], r['y'], r['pad']
    blocks, seqs, _, width = u_ref.shape
    toks = blocks * 8

    def one_seq(s, carry):
        u = u_ref[:, s].reshape(toks, width)
        pad[8:8 + toks, :] = u
        for j in range(CONV_WIDTH - 1):
            pad[5 + j:6 + j, :] = r['conv_state'][s, j].astype(F32)[layer:layer + 1]
        r['o_conv'][s] = u[toks - 3:, :].astype(BF16)
        total = jnp.zeros((toks, width), F32)
        for j in range(CONV_WIDTH):
            total = total + pad[5 + j:5 + j + toks, :] * r['conv_w'][layer, j:j + 1, :].astype(F32)
        row_of = lambda key: r[key][layer:layer + 1, :].astype(F32)
        conv = (total + row_of('conv_b')).astype(BF16)
        gate_r = jax.nn.sigmoid(jnp.dot(conv, r['w_a'][layer, 0], preferred_element_type=F32) + row_of('b_a'))
        gate_i = jax.nn.sigmoid(jnp.dot(conv, r['w_i'][layer, 0], preferred_element_type=F32) + row_of('b_i'))
        decay = jnp.exp(-8.0 * gate_r * row_of('soft'))
        reset = column_of(r['seg_pos'][pl.ds(s, 1), :]) == 0
        mult = jnp.where(reset, 1.0, jnp.sqrt(1.0 - decay * decay))
        decay = jnp.where(reset, 0.0, decay)
        drive = conv.astype(F32) * gate_i * mult
        a = decay.reshape(blocks, 8, width)
        b = drive.reshape(blocks, 8, width)
        row = lax.broadcasted_iota(jnp.int32, (blocks, 8, width), 1)
        for k in (1, 2, 4):
            inside = row >= k
            a_sh = jnp.where(inside, pltpu.roll(a, k, 1), 1.0)
            b_sh = jnp.where(inside, pltpu.roll(b, k, 1), 0.0)
            b = a * b_sh + b
            a = a * a_sh
        state = r['lru_state'][s, layer:layer + 1, :]
        for blk in range(blocks):
            h = a[blk] * state + b[blk]
            state = h[7:8, :]
            u_ref[blk, s] = h * y_ref[blk, s]
        r['o_lru'][pl.ds(s, 1), :] = state
        return carry
    lax.fori_loop(0, seqs, one_seq, 0)


def comm_kernel(plan, tp, names, outs, scratch, *refs):
    r = dict(zip(names + outs + scratch, refs))
    x_ref = r['x']
    rows, dim = x_ref.shape
    net = Net(tp, rows, dim, r)
    net.greet()
    loads = [[] for _ in plan]
    count = 0
    for i, step in enumerate(plan):
        for key, src, layer in step['loads']:
            view = r[src] if layer is None else r[src].at[layer]
            loads[i].append((key, pltpu.make_async_copy(view, r[key], r['w_sem'].at[count])))
            count += 1
    used = set()
    for step in loads:
        for key, copy in step:
            if key not in used:
                used.add(key)
                copy.start()

    def refill(i):
        for key, _ in loads[i]:
            later = [copy for step in loads[i + 1:] for k, copy in step if k == key]
            if later:
                later[0].start()

    xbuf = r['xbuf']
    xbuf[...] = x_ref[...]
    groups = range(net.groups)

    def enter(idx, steps):
        def norm(group):
            span = pl.ds(group * ROW_TILE, ROW_TILE)
            h = xbuf[span, :].astype(F32)
            inv = lax.rsqrt(jnp.mean(h * h, axis=-1, keepdims=True) + 1e-6)
            r['g'][net.core, span, :] = (h * inv * (1.0 + r['norm'][idx:idx + 1, :].astype(F32))).astype(BF16)
        if steps is None:
            for group in groups:
                norm(group)
            net.meet()
            for group in groups:
                net.gather_start(group)
        else:
            for group in steps:
                norm(group)
                net.gather_start(group)
            net.reduce_end()

    def finish_with(bias_ref, idx):
        def finish(span, total):
            xbuf[span] = (xbuf[span].astype(F32) + total + bias_ref[idx:idx + 1, span[1]].astype(F32)).astype(BF16)
        return finish

    def block_of(first, last):
        return r['g'][2 * first:2 * last].reshape((last - first) * 2 * rows, dim)

    def wait_loads(i):
        pending = list(loads[i])

        def wait():
            while pending:
                pending.pop()[1].wait()
        return wait

    reduction = None
    for i, step in enumerate(plan):
        kind, idx = step['kind'], step['idx']
        ready = wait_loads(i)
        if kind == 'pre':
            ready()
            source = r['mid'] if 'mid' in r else r['u']
            r['apre'][...] = source[...].reshape(r['apre'].shape).astype(BF16)
            if i == 0:
                net.meet()

            def lhs_pre(slot, core):
                blk = 2 * net.abs_chip(SLOT_REL[slot]) + core
                return r['apre'][pl.ds(pl.multiple_of(blk * rows, 16), rows), :]
            reduction = net.reduce(lhs_pre, r['w_pre'], finish_with(r['b_pre'], idx))
            owner = i
        elif kind == 'mlp':
            def mlp_pass(first, last, ready=ready, m=idx):
                ready()
                width = 2 * (last - first)

                def body(t, carry):
                    cols = pl.ds(pl.multiple_of(t * 256, 256), 256)
                    lhs = block_of(first, last)
                    h1 = jnp.dot(lhs, r['w_1s'][:, cols], preferred_element_type=F32) + r['b_1'][m:m + 1, cols].astype(F32)
                    h2 = jnp.dot(lhs, r['w_2s'][:, cols], preferred_element_type=F32) + r['b_2'][m:m + 1, cols].astype(F32)
                    act = (jax.nn.gelu(h1, approximate=True) * h2).astype(BF16)
                    r['act'][2 * first:2 * last, :, cols] = act.reshape(width, rows, 256)
                    return carry
                lax.fori_loop(0, r['w_1s'].shape[1] // 256, body, 0)
            enter(2 * idx + 1, reduction)
            refill(owner)
            net.gather(mlp_pass)
            reduction = net.reduce(lambda slot, core: r['act'][2 * slot + core], r['w_ds'], finish_with(r['b_d'], idx), functools.partial(net.gather_end, mlp_pass))
            owner = i
        else:
            def post_pass(first, last, ready=ready, kind=kind, layer=idx):
                ready()
                lhs = block_of(first, last)
                chips = [net.abs_chip(SLOT_REL[s]) for s in range(first, last)]

                def put(ref, value, rope=False):
                    for n, chip in enumerate(chips):
                        v = value[n * 2 * rows:(n + 1) * 2 * rows]
                        if rope:
                            span = pl.ds(pl.multiple_of(chip * 2 * rows, 16), 2 * rows)
                            lo = v[:, :ROPE_DIM]
                            lo = lo * r['cos'][span, :] + pltpu.roll(lo, ROPE_DIM // 2, 1) * r['sin'][span, :]
                            v = jnp.concatenate([lo, v[:, ROPE_DIM:]], axis=1)
                        ref[pl.ds(2 * chip, 2)] = v.astype(BF16).astype(F32).reshape((2,) + ref.shape[1:])
                if kind == 'rec':
                    put(r['u'], jnp.dot(lhs, r['p_0'][...], preferred_element_type=F32) + r['b_x'][layer:layer + 1, :].astype(F32))
                    put(r['y'], jax.nn.gelu(jnp.dot(lhs, r['p_1'][...], preferred_element_type=F32) + r['b_y'][layer:layer + 1, :].astype(F32), approximate=True))
                else:
                    put(r['o_q'], jnp.dot(lhs, r['p_0'][...], preferred_element_type=F32), True)
                    put(r['o_k'], jnp.dot(lhs, r['p_1'][...], preferred_element_type=F32), True)
                    put(r['o_v'], jnp.dot(lhs, r['p_2'][...], preferred_element_type=F32))
            enter(4 if kind == 'attn' else 2 * idx, reduction)
            if reduction is not None:
                refill(owner)
            net.gather(post_pass)
            net.gather_end(post_pass)
            refill(i)
            reduction = None
            if kind == 'rec':
                recurrence(idx, r)
    if reduction is not None:
        for _ in reduction:
            pass
        net.reduce_end()
    r['o_x'][...] = xbuf[...]


def comm_call(tp, ident, x, plan, small, large, outs, extra):
    rows, dim = x.shape
    vmem, hbm = pl.BlockSpec(memory_space=pltpu.VMEM), pl.BlockSpec(memory_space=pl.ANY)
    small = dict(x=x, **small)
    names = list(small) + list(large)
    outs = dict(o_x=jax.ShapeDtypeStruct((rows, dim), BF16), **outs)
    scratch = dict(extra)
    flops = 0
    total = 0
    for step in plan:
        for key, src, layer in step['loads']:
            shape = large[src].shape[-2:]
            scratch.setdefault(key, pltpu.VMEM(shape, BF16))
            flops += 2 * tp * rows * shape[0] * shape[1]
            total += 1
    scratch['pown'] = pltpu.VMEM((8, rows, dim), F32)
    scratch['dsend'] = pltpu.VMEM((8, rows, dim), BF16)
    scratch['drecv'] = pltpu.VMEM((8, rows, dim), BF16)
    scratch['zsend'] = pltpu.VMEM((2, 4, rows, dim), BF16)
    scratch['zrecv'] = pltpu.VMEM((2, 4, rows, dim), BF16)
    scratch['act'] = pltpu.VMEM((tp, rows, scratch['w_1s'].shape[1]), BF16)
    scratch['apre'] = pltpu.VMEM((tp * rows, scratch['w_pre'].shape[0]), BF16)
    scratch['g'] = pltpu.VMEM((tp, rows, dim), BF16)
    scratch['xbuf'] = pltpu.VMEM((rows, dim), BF16)
    for key in ('ag_z', 'rs_z', 'send_z', 'give_z'):
        scratch[key] = pltpu.SemaphoreType.DMA((2, 4, 2, rows // ROW_TILE))
    for key in ('ag_d', 'rs_d', 'send_d', 'give_d'):
        scratch[key] = pltpu.SemaphoreType.DMA((8, 2, rows // ROW_TILE))
    scratch['w_sem'] = pltpu.SemaphoreType.DMA((total,))
    result = pl.pallas_call(
        functools.partial(comm_kernel, plan, tp, names, list(outs), list(scratch)),
        out_shape=tuple(outs.values()),
        in_specs=[vmem] * len(small) + [hbm] * len(large),
        out_specs=tuple(vmem for _ in outs),
        scratch_shapes=list(scratch.values()),
        compiler_params=pltpu.CompilerParams(collective_id=ident, has_side_effects=True, vmem_limit_bytes=67 * 1000 * 1000),
        cost_estimate=pl.CostEstimate(flops=flops, bytes_accessed=flops // 1500, transcendentals=0),
        name='ring_' + str(ident),
    )(*small.values(), *large.values())
    return dict(zip(outs, result))


def attn_kernel(q_ref, k_ref, v_ref, kc_ref, vc_ref, slot_ref, pos_ref, o_ref, ko_ref, vo_ref, so_ref):
    blocks, _, _, width = q_ref.shape
    toks = blocks * 8
    q = (q_ref[...].reshape(toks, width) * SCORE_SCALE).astype(BF16)
    kn = k_ref[...].reshape(toks, width).astype(BF16)
    vn = v_ref[...].reshape(toks, width).astype(BF16)
    kc, vc = kc_ref[0], vc_ref[0]
    seq = pl.ds(pl.program_id(0), 1)
    slot, pos_row = slot_ref[seq, :], pos_ref[seq, :]
    pos_mat = jnp.broadcast_to(pos_row, (toks, toks))
    pos_mat_t = pos_mat.T
    pos_col = pos_mat_t[:, :1]
    row_i = lax.broadcasted_iota(jnp.int32, (toks, toks), 0)
    col_i = lax.broadcasted_iota(jnp.int32, (toks, toks), 1)
    doc_col = jnp.sum(jnp.where((pos_mat == 0) & (col_i <= row_i), 1.0, 0.0), axis=1, keepdims=True)
    doc_row = jnp.sum(jnp.where((pos_mat_t == 0) & (row_i <= col_i), 1.0, 0.0), axis=0, keepdims=True)
    contract = (((1,), (1,)), ((), ()))
    diff_old = jnp.where(doc_col == 0, pos_col, -(2 ** 30)) - jnp.where(slot >= 0, slot, -(2 ** 29))
    keep_old = (diff_old >= 0) & (diff_old < WINDOW)
    diff_new = pos_col - pos_row
    keep_new = (diff_new >= 0) & (diff_new < WINDOW) & (doc_col == doc_row)
    s_old = jnp.where(keep_old, lax.dot_general(q, kc, contract, preferred_element_type=F32), NEG_BIG)
    s_new = jnp.where(keep_new, lax.dot_general(q, kn, contract, preferred_element_type=F32), NEG_BIG)
    top = jnp.maximum(jnp.max(s_old, axis=-1, keepdims=True), jnp.max(s_new, axis=-1, keepdims=True))
    e_old = jnp.exp(s_old - top)
    e_new = jnp.exp(s_new - top)
    denom = jnp.sum(e_old, axis=-1, keepdims=True) + jnp.sum(e_new, axis=-1, keepdims=True)
    inv = 1.0 / denom
    out = jnp.dot((e_old * inv).astype(BF16), vc, preferred_element_type=F32) + jnp.dot((e_new * inv).astype(BF16), vn, preferred_element_type=F32)
    o_ref[...] = out.astype(BF16).astype(F32).reshape(o_ref.shape)
    window = kc.shape[0]
    target_row = lax.rem(pos_row, window)
    target_col = lax.rem(pos_col, window)
    hit = lax.broadcasted_iota(jnp.int32, (window, toks), 0) == target_row
    pick = jnp.where(hit, 1.0, 0.0)
    any_hit = jnp.max(pick, axis=1, keepdims=True) > 0.0
    pick = pick.astype(BF16)
    ko_ref[0] = jnp.where(any_hit, jnp.dot(pick, kn, preferred_element_type=F32), kc.astype(F32)).astype(BF16)
    vo_ref[0] = jnp.where(any_hit, jnp.dot(pick, vn, preferred_element_type=F32), vc.astype(F32)).astype(BF16)
    hit_t = lax.broadcasted_iota(jnp.int32, (toks, window), 1) == target_col
    newest = jnp.max(jnp.where(hit_t, pos_col, -1), axis=0, keepdims=True)
    so_ref[seq, :] = jnp.where(newest >= 0, newest, slot)


def attn_call(q, k, v, k_cache, v_cache, slot_pos, seg_pos):
    seqs, toks = seg_pos.shape
    width = q.shape[-1]
    blocks = toks // 8
    window = k_cache.shape[1]
    shape4 = (blocks, seqs, 8, width)
    tok_spec = pl.BlockSpec((blocks, 1, 8, width), lambda s: (0, s, 0, 0))
    cache_spec = pl.BlockSpec((1, window, width), lambda s: (s, 0, 0))
    row_spec = lambda n: pl.BlockSpec((seqs, n), lambda s: (0, 0))
    out, k_out, v_out, slot_out = pl.pallas_call(
        attn_kernel,
        grid=(seqs,),
        out_shape=(jax.ShapeDtypeStruct(shape4, F32), jax.ShapeDtypeStruct(k_cache.shape, BF16), jax.ShapeDtypeStruct(v_cache.shape, BF16), jax.ShapeDtypeStruct((seqs, window), jnp.int32)),
        in_specs=[tok_spec, tok_spec, tok_spec, cache_spec, cache_spec, row_spec(window), row_spec(toks)],
        out_specs=(tok_spec, cache_spec, cache_spec, row_spec(window)),
        cost_estimate=pl.CostEstimate(flops=8 * seqs * toks * window * width, bytes_accessed=8 * seqs * window * width, transcendentals=0),
        name='attention',
    )(q, k, v, k_cache, v_cache, slot_pos, seg_pos)
    return out, k_out, v_out, slot_out


def solution(mesh):
    tp = mesh.shape['tp']

    def device_body(x_in, seg_pos, conv_state, lru_state, k_cache, v_cache, slot_pos, norm_scale, w_x, b_x, w_y, b_y, conv_w, conv_b, w_a, b_a, w_i, b_i, a_param, w_out, b_out, w_q, w_k, w_v, w_o, b_o, w_1, b_1, w_2, b_2, w_d, b_d):
        seqs, toks = seg_pos.shape
        dim = x_in.shape[-1]
        x = x_in.reshape(-1, dim)
        soft = jax.nn.softplus(a_param)
        half = ROPE_DIM // 2
        timescale = 10000.0 ** (2.0 * jnp.arange(half).astype(F32) / ROPE_DIM)
        order = seg_pos.reshape(seqs, toks // 8, 8).swapaxes(0, 1).reshape(-1)
        angle = order[:, None].astype(F32) / timescale
        sin, cos = jnp.sin(angle), jnp.cos(angle)
        cos2 = jnp.concatenate([cos, cos], axis=1)
        sin2 = jnp.concatenate([-sin, sin], axis=1)

        width = w_q.shape[-1]
        shape4 = (tp, seqs, 8, width)
        tall = jax.ShapeDtypeStruct(shape4, F32)

        def mlp_step(m):
            return dict(kind='mlp', idx=m, loads=(('w_1s', 'w_1', m), ('w_2s', 'w_2', m), ('w_ds', 'w_d', m)))

        def rec_step(layer):
            return dict(kind='rec', idx=layer, loads=(('p_0', 'w_x', layer), ('p_1', 'w_y', layer)))

        def out_step(layer):
            return dict(kind='pre', idx=layer, loads=(('w_pre', 'w_out', layer),))
        mlp_small = dict(norm=norm_scale, b_1=b_1, b_2=b_2, b_d=b_d)
        mlp_large = dict(w_1=w_1, w_2=w_2, w_d=w_d)
        rec_small = dict(mlp_small, b_pre=b_out, b_x=b_x, b_y=b_y, seg_pos=seg_pos, conv_state=conv_state.transpose(1, 2, 0, 3),
                         lru_state=lru_state.swapaxes(0, 1), conv_w=conv_w, conv_b=conv_b, w_a=w_a, b_a=b_a, w_i=w_i, b_i=b_i, soft=soft)
        rec_large = dict(mlp_large, w_x=w_x, w_y=w_y, w_out=w_out)
        rec_outs = dict(o_conv=jax.ShapeDtypeStruct(conv_state.shape[1:], BF16), o_lru=jax.ShapeDtypeStruct(lru_state.shape[1:], F32))
        work = dict(u=pltpu.VMEM(shape4, F32), y=pltpu.VMEM(shape4, F32), pad=pltpu.VMEM((toks + 8, width), F32))
        zero = comm_call(tp, 0, x, (rec_step(0), out_step(0), mlp_step(0)), rec_small, rec_large, rec_outs, work)
        one = comm_call(
            tp, 1, zero['o_x'],
            (rec_step(1), out_step(1), mlp_step(1), dict(kind='attn', idx=0, loads=(('p_0', 'w_q', None), ('p_1', 'w_k', None), ('p_2', 'w_v', None)))),
            dict(rec_small, cos=cos2, sin=sin2), dict(rec_large, w_q=w_q, w_k=w_k, w_v=w_v), dict(rec_outs, o_q=tall, o_k=tall, o_v=tall), work)
        mid, k_out, v_out, slot_out = attn_call(one['o_q'], one['o_k'], one['o_v'], k_cache, v_cache, slot_pos, seg_pos)
        last = comm_call(
            tp, 2, one['o_x'], (dict(kind='pre', idx=0, loads=(('w_pre', 'w_o', None),)), mlp_step(2)),
            dict(mlp_small, b_pre=b_o[None, :], mid=mid), dict(mlp_large, w_o=w_o), {}, {})
        conv_out = jnp.stack([zero['o_conv'], one['o_conv']], axis=2).transpose(2, 0, 1, 3)
        lru_out = jnp.stack([zero['o_lru'], one['o_lru']], axis=1).swapaxes(0, 1)
        return last['o_x'].reshape(x_in.shape), conv_out, lru_out, k_out, v_out, slot_out

    col_spec = P(None, None, 'tp')
    vec_spec = P(None, 'tp')
    block_spec = P(None, 'tp', None, None)
    row_spec = P(None, 'tp', None)
    cache_spec = P('dp', None, None)
    arg_specs = (P('dp', 'tp', None), P('dp', None), P(None, 'dp', None, 'tp'), P(None, 'dp', 'tp'), cache_spec, cache_spec, P('dp', None), P(), col_spec, vec_spec, col_spec, vec_spec, col_spec, vec_spec, block_spec, vec_spec, block_spec, vec_spec, vec_spec, row_spec, P(), P(None, 'tp'), P(), P(), P('tp', None), P(), col_spec, vec_spec, col_spec, vec_spec, row_spec, P())
    result_specs = (P('dp', 'tp', None), P(None, 'dp', None, 'tp'), P(None, 'dp', 'tp'), cache_spec, cache_spec, P('dp', None))
    return jax.shard_map(device_body, mesh=mesh, in_specs=arg_specs, out_specs=result_specs, check_vma=False)
```
